32 devices in a mesh: shard: 8 (over z, x), width: 4 (over y, core).
Axes of the slice: x: 2, y: 2, z: 4, core: 2. Of those that a mesh axis runs over, the one named last changes fastest.
Arguments:
- w_gate: bfloat16 [2048, 8192], P('shard', 'width'), may hold values from -0.125 to 0.125
- low_gate: bfloat16 [2048, 64], P('shard'), may hold values from -0.125 to 0.125
- high_gate: bfloat16 [64, 8192], P(None, 'width'), may hold values from -0.75 to 0.75
- w_up: bfloat16 [2048, 8192], P('shard', 'width'), may hold values from -0.125 to 0.125
- low_up: bfloat16 [2048, 64], P('shard'), may hold values from -0.125 to 0.125
- high_up: bfloat16 [64, 8192], P(None, 'width'), may hold values from -0.75 to 0.75
- w_down: bfloat16 [8192, 2048], P('width', 'shard'), may hold values from -0.0625 to 0.0625
- low_down: bfloat16 [8192, 64], P('width'), may hold values from -0.0625 to 0.0625
- high_down: bfloat16 [64, 2048], P(None, 'shard'), may hold values from -0.75 to 0.75
- norm_train: float32 [2048], P(('shard', 'width')), may hold values from 0.25 to 1.75
- norm_step: float32 [2048], P(('shard', 'width')), may hold values from -0.3 to 0.3
Outputs:
- serve_gate: bfloat16 [8192, 2048], P('width')
- serve_up: bfloat16 [8192, 2048], P('width')
- serve_down: bfloat16 [2048, 8192], P(None, 'width')
- serve_norm: bfloat16 [2048], replicated
The draws below stay inside these ranges and needn't reach their ends.
All inputs are finite; a program needn't handle non-finite values.
Results may differ from the reference program's by a relative error of at most 0.001.
Values may be sent and summed in bfloat16 or wider, within the bound.
A program may use at most 128 MiB of HBM per device.

```python
import jax
import jax.numpy as jnp

D_MODEL = 2048
D_INNER = 8192
RANK = 64


def level_of(own_key, extent, cuts, smallest, largest):
    factor_of, own = 1.0, jax.random.fold_in(own_key, 6)
    for dim, shards_of in cuts:
        steps = jnp.exp(jax.random.uniform(jax.random.fold_in(own, dim), (shards_of,), jnp.float32, smallest / len(cuts), largest / len(cuts)))
        factor_of = factor_of * jnp.repeat(steps, extent[dim] // shards_of).reshape([-1 if axis == dim else 1 for axis in range(len(extent))])
    return factor_of


def gaussian(stream_key, extent, deviation, reach, pieces=(), dtype=jnp.bfloat16):
    drawn = deviation * jax.random.normal(stream_key, extent, jnp.float32)
    if pieces:
        drawn = drawn * level_of(stream_key, extent, pieces, -0.22, 0.18)
    return jnp.clip(drawn, -reach, reach).astype(dtype)


def setup_inputs(seed: int = 0) -> dict:
    key_list = jax.random.split(jax.random.key(seed), 12)
    w_gate = gaussian(key_list[0], (D_MODEL, D_INNER), D_MODEL ** -0.5, 0.125, ((0, 8), (1, 4)))
    low_gate = gaussian(key_list[1], (D_MODEL, RANK), D_MODEL ** -0.5, 0.125, ((0, 8),))
    high_gate = gaussian(key_list[2], (RANK, D_INNER), RANK ** -0.5, 0.75, ((1, 4),))
    w_up = gaussian(key_list[3], (D_MODEL, D_INNER), D_MODEL ** -0.5, 0.125, ((0, 8), (1, 4)))
    low_up = gaussian(key_list[4], (D_MODEL, RANK), D_MODEL ** -0.5, 0.125, ((0, 8),))
    high_up = gaussian(key_list[5], (RANK, D_INNER), RANK ** -0.5, 0.75, ((1, 4),))
    w_down = gaussian(key_list[6], (D_INNER, D_MODEL), D_INNER ** -0.5, 0.0625, ((0, 4), (1, 8)))
    low_down = gaussian(key_list[7], (D_INNER, RANK), D_INNER ** -0.5, 0.0625, ((0, 4),))
    high_down = gaussian(key_list[8], (RANK, D_MODEL), RANK ** -0.5, 0.75, ((1, 8),))
    norm_train = jnp.clip(1.0 + 0.15 * jax.random.normal(key_list[9], (D_MODEL,), jnp.float32), 0.25, 1.75)
    norm_step = jnp.clip(jax.random.uniform(key_list[10], (D_MODEL,), jnp.float32, -0.3, 0.3) * level_of(key_list[10], (D_MODEL,), ((0, 32),), -0.4, 0.0), -0.3, 0.3)
    return {"w_gate": w_gate, "low_gate": low_gate, "high_gate": high_gate, "w_up": w_up, "low_up": low_up, "high_up": high_up, "w_down": w_down, "low_down": low_down, "high_down": high_down, "norm_train": norm_train, "norm_step": norm_step}


mix_rate = 2.0


def reference(w_gate, low_gate, high_gate, w_up, low_up, high_up, w_down, low_down, high_down, norm_train, norm_step):
    fresh_gate = w_gate.astype(jnp.float32) + mix_rate * jnp.dot(low_gate, high_gate, preferred_element_type=jnp.float32)
    fresh_up = w_up.astype(jnp.float32) + mix_rate * jnp.dot(low_up, high_up, preferred_element_type=jnp.float32)
    fresh_down = w_down.astype(jnp.float32) + mix_rate * jnp.dot(low_down, high_down, preferred_element_type=jnp.float32)
    serve_gate = fresh_gate.T.astype(jnp.bfloat16)
    serve_up = fresh_up.T.astype(jnp.bfloat16)
    serve_down = fresh_down.T.astype(jnp.bfloat16)
    serve_norm = (norm_train + norm_step).astype(jnp.bfloat16)
    return serve_gate, serve_up, serve_down, serve_norm
```

```python
import functools

import jax
import jax.numpy as jnp
from jax import lax
from jax.experimental import pallas as pl
from jax.experimental.pallas import tpu as pltpu
from jax.sharding import PartitionSpec as P

mix_rate = 2.0
MESH = pl.DeviceIdType.MESH
X = 2
LANES = 128

CUTS = 4
LINE = ((0, 0), (0, 1), (1, 0), (0, 2), (1, 1), (2, 0), (0, 3), (1, 2), (2, 1), (2, 2))
PAIR = ((1, 3), (2, 3))
ORDER = LINE[:2] + PAIR[:1] + LINE[2:6] + PAIR[1:] + LINE[6:]
UP, DOWN, SIDE = 0, 1, 2
WAYS = 3
N_PIECES = 3 * CUTS


def merged(w, low, high):
    fresh = w.astype(jnp.float32) + mix_rate * jnp.dot(
        low, high, preferred_element_type=jnp.float32
    )
    return fresh.astype(jnp.bfloat16)


def when(cond, fn):
    if cond is None:
        fn()
    else:
        pl.when(cond)(fn)


def both(a, b):
    if a is None:
        return b
    if b is None:
        return a
    return jnp.logical_and(a, b)


def gather_kernel(
    shards, widths,
    w_gate, low_gate, high_gate, w_up, low_up, high_up, w_down, low_down, high_down, train, step,
    o_gate, o_up, o_down, o_norm,
    v_gate, v_up, v_down, v_low_gate, v_low_up, v_low_down, v_high_gate, v_high_up, v_high_down,
    v_train, v_step, l_gate, l_up, h_down,
    send_sem, recv_sem, norm_send, norm_recv, load_sem, small_sem,
):
    lines = shards // X
    me, w = lax.axis_index("shard"), lax.axis_index("width")
    z, x = me // X, me % X
    partner = z * X + (1 - x)
    outs = (o_gate, o_up, o_down)
    big = ((w_gate, v_gate), (w_up, v_up), (w_down, v_down))
    wide = w_gate.shape[0]
    cut = w_gate.shape[1] // CUTS

    def load(c):
        t, h = c
        src, dst = big[t]
        at = (slice(None), pl.ds(h * cut, cut)) if t < 2 else (pl.ds(h * cut, cut), slice(None))
        return pltpu.make_async_copy(src.at[at], dst.at[at], load_sem.at[t * CUTS + h])

    smalls = [
        (low_gate, v_low_gate), (high_gate, v_high_gate),
        (low_up, v_low_up), (high_up, v_high_up),
        (low_down, v_low_down), (high_down, v_high_down),
        (train, v_train), (step, v_step),
    ]
    small = [pltpu.make_async_copy(a, b, small_sem.at[i]) for i, (a, b) in enumerate(smalls)]
    first = {0: small[0:2], 1: small[2:4], 2: small[4:6]}
    started = set()
    for c in ORDER:
        if c[0] not in started:
            started.add(c[0])
            for copy in first[c[0]]:
                copy.start()
        load(c).start()
    for copy in small[6:]:
        copy.start()

    def target(way):
        return {UP: me + X, DOWN: me - X, SIDE: partner}[way]

    def has(way):
        return {UP: z + 1 < lines, DOWN: z > 0, SIDE: None}[way]

    barrier = pltpu.get_barrier_semaphore()
    peers = [lax.rem(w + k, widths) for k in range(1, widths)]
    for way in (UP, DOWN, SIDE):
        when(
            has(way),
            lambda way=way: pl.semaphore_signal(
                barrier, inc=1, device_id=(target(way), w), device_id_type=MESH
            ),
        )
    for p in peers:
        pl.semaphore_signal(barrier, inc=1, device_id=(me, p), device_id_type=MESH)

    def place(s, c):
        t, h = c
        at = pl.ds(pl.multiple_of(s * wide, wide), wide)
        return outs[t].at[pl.ds(h * cut, cut), at] if t < 2 else outs[t].at[at, pl.ds(h * cut, cut)]

    slots = {}
    sends = []

    def index(c):
        return c[0] * CUTS + c[1]

    def send(way, s, c, cond):
        slot = slots.get(way, 0)
        slots[way] = slot + 1

        def make():
            return pltpu.make_async_remote_copy(
                src_ref=place(s, c),
                dst_ref=place(s, c),
                send_sem=send_sem.at[way, slot],
                recv_sem=recv_sem.at[s * N_PIECES + index(c)],
                device_id=(target(way), w),
                device_id_type=MESH,
            )

        full = both(cond, has(way))
        when(full, lambda: make().start())
        sends.append((full, lambda: make().wait_send()))

    def arrive(s, c, cond=None):
        when(
            cond,
            lambda: pltpu.make_async_remote_copy(
                src_ref=place(s, c),
                dst_ref=place(s, c),
                send_sem=send_sem.at[0, 0],
                recv_sem=recv_sem.at[s * N_PIECES + index(c)],
                device_id=(partner, w),
                device_id_type=MESH,
            ).wait_recv(),
        )

    seen = set()

    def compute(c):
        t, h = c
        if t not in seen:
            seen.add(t)
            for copy in first[t]:
                copy.wait()
            if t == 0:
                l_gate[...] = v_low_gate[...].T
            elif t == 1:
                l_up[...] = v_low_up[...].T
            else:
                h_down[...] = v_high_down[...].T
        load(c).wait()
        columns = pl.ds(pl.multiple_of(me * wide, wide), wide)

        @pl.loop(0, cut // LANES)
        def _(i):
            at = pl.ds(pl.multiple_of(h * cut + i * LANES, LANES), LANES)
            if t < 2:
                block, low, high = ((v_gate, l_gate, v_high_gate), (v_up, l_up, v_high_up))[t]
                outs[t][at, columns] = merged(block[:, at], low[...], high[:, at]).T
            else:
                o_down[columns, at] = merged(v_down[at, :].T, h_down[...], v_low_down[:, at])

    def send_own(c):
        if c in LINE:
            send(UP, me, c, None)
            send(DOWN, me, c, None)
        send(SIDE, me, c, None)

    compute(ORDER[0])
    inner = jnp.logical_and(z > 0, z + 1 < lines)
    pl.when(inner)(lambda: pl.semaphore_wait(barrier, widths + 2))
    ends = widths + (1 if lines > 1 else 0)
    pl.when(jnp.logical_not(inner))(lambda: pl.semaphore_wait(barrier, ends))
    for k, c in enumerate(ORDER):
        if k:
            compute(c)
        send_own(c)

    def norm_rows(begin, count):
        return o_norm.at[pl.ds(begin, count)]

    def norm_copy(begin, count, sem, rsem, dev):
        return pltpu.make_async_remote_copy(
            src_ref=norm_rows(begin, count), dst_ref=norm_rows(begin, count),
            send_sem=norm_send.at[sem], recv_sem=norm_recv.at[rsem],
            device_id=dev, device_id_type=MESH,
        )

    for copy in small[6:]:
        copy.wait()
    gain = v_train[...] + v_step[...]
    row = jnp.concatenate([gain] * (LANES // gain.shape[1]), axis=1)
    o_norm[pl.ds(me * widths + w, 1)] = row.reshape(1, 1, LANES)
    tile_of = lambda k: norm_copy(me * widths + w, 1, k - 1, k - 1, (me, peers[k - 1]))
    for k in range(1, widths):
        tile_of(k).start()
    side_at = widths - 1
    norm_side = lambda s: norm_copy(s * widths, widths, side_at, side_at, (partner, w))

    def norm_gather():
        for k in range(1, widths):
            source = lax.rem(w + widths - k, widths)
            norm_copy(me * widths + source, 1, k - 1, k - 1, (me, peers[k - 1])).wait_recv()
        norm_side(me).start()

    for d in range(1, lines):
        for c in LINE:
            for way, s, cond in (
                (UP, me - d * X, z >= d),
                (DOWN, me + d * X, z + d < lines),
            ):
                arrive(s, c, cond)
                send(way, s, c, cond)
                send(SIDE, s, c, cond)
        if d == 1:
            norm_gather()
    if lines == 1:
        norm_gather()

    for c in PAIR:
        arrive(partner, c)
    norm_side(partner).wait_recv()

    def norm_pair(way, plane):
        rows = X * widths
        at = widths + way * lines
        return norm_copy(
            plane * rows, rows, at + (plane - z) * (1 - 2 * way) * -1, widths + plane, (target(way), w)
        )

    for d in range(lines):
        for way, plane, cond in (
            (UP, z - d, z >= d),
            (DOWN, z + d, z + d < lines),
        ):
            if d == 0:
                cond = None
            full = both(cond, has(way))
            if d > 0:
                when(cond, lambda way=way, plane=plane: norm_pair(way, plane).wait_recv())
            when(full, lambda way=way, plane=plane: norm_pair(way, plane).start())
            sends.append((full, lambda way=way, plane=plane: norm_pair(way, plane).wait_send()))
            for c in PAIR:
                for j in range(X):
                    s = (me if j == 0 else partner) if d == 0 else plane * X + j
                    if d > 0:
                        arrive(s, c, cond)
                    send(way, s, c, cond)

    for c in LINE:
        arrive(partner, c)
    for d in range(1, lines):
        for c in LINE:
            arrive(partner - d * X, c, z >= d)
            arrive(partner + d * X, c, z + d < lines)
    for k in range(1, widths):
        tile_of(k).wait_send()
    norm_side(me).wait_send()
    for cond, wait in sends:
        when(cond, wait)


def gather_all(shards, widths, args):
    lines = shards // X
    w_gate, low_gate, high_gate, w_up, low_up, high_up, w_down, low_down, high_down, train, step = args
    hbm = pl.BlockSpec(memory_space=pltpu.HBM)
    vmem = pl.BlockSpec(memory_space=pltpu.VMEM)
    like = lambda a: pltpu.VMEM(a.shape, a.dtype)
    flip = lambda a: pltpu.VMEM(a.shape[::-1], a.dtype)
    wide, tall = w_gate.shape
    full = pltpu.VMEM((tall, shards * wide), w_gate.dtype)
    long = len(LINE) * lines + len(PAIR) * lines * X
    return pl.pallas_call(
        functools.partial(gather_kernel, shards, widths),
        out_shape=(
            full, full,
            pltpu.VMEM((shards * wide, tall), w_down.dtype),
            pltpu.VMEM((shards * widths, 1, LANES), train.dtype),
        ),
        in_specs=[hbm] * len(args),
        out_specs=(vmem,) * 4,
        scratch_shapes=[
            like(w_gate), like(w_up), like(w_down),
            like(low_gate), like(low_up), like(low_down),
            like(high_gate), like(high_up), like(high_down),
            like(train), like(step),
            flip(low_gate), flip(low_up), flip(high_down),
            pltpu.SemaphoreType.DMA((WAYS, max(long, N_PIECES + 2 * len(LINE) * lines))),
            pltpu.SemaphoreType.DMA((shards * N_PIECES,)),
            pltpu.SemaphoreType.DMA((widths + 2 * lines,)),
            pltpu.SemaphoreType.DMA((widths + lines,)),
            pltpu.SemaphoreType.DMA((N_PIECES,)),
            pltpu.SemaphoreType.DMA((8,)),
        ],
        compiler_params=pltpu.CompilerParams(collective_id=0, has_side_effects=True, vmem_limit_bytes=16 * 2**20),
    )(*(pltpu.with_memory_space_constraint(a, pltpu.HBM) for a in args))


def write_kernel(gate, up, down, rows, o_gate, o_up, o_down, o_norm, norm, sem):
    pairs = ((gate, o_gate), (up, o_up), (down, o_down))
    copies = [pltpu.make_async_copy(a, b, sem.at[i]) for i, (a, b) in enumerate(pairs)]
    for copy in copies:
        copy.start()
    per = rows.shape[1]
    lane = lax.broadcasted_iota(jnp.int32, norm.shape, 1) // (LANES // per)
    line = rows[:, 0, :]
    for j in range(1, per):
        line = jnp.where(lane == j, rows[:, j, :], line)
    norm[...] = line.astype(norm.dtype)
    copy = pltpu.make_async_copy(norm, o_norm, sem.at[3])
    copy.start()
    copy.wait()
    for copy in copies:
        copy.wait()


def write_out(gate, up, down, rows):
    any_ = pl.BlockSpec(memory_space=pl.ANY)
    vmem = pl.BlockSpec(memory_space=pltpu.VMEM)
    norm = (rows.shape[0], LANES)
    return pl.pallas_call(
        write_kernel,
        out_shape=tuple(jax.ShapeDtypeStruct(a.shape, a.dtype) for a in (gate, up, down))
        + (jax.ShapeDtypeStruct(norm, jnp.bfloat16),),
        in_specs=[any_] * 3 + [vmem],
        out_specs=(any_,) * 4,
        scratch_shapes=[pltpu.VMEM(norm, jnp.bfloat16), pltpu.SemaphoreType.DMA((4,))],
        compiler_params=pltpu.CompilerParams(vmem_limit_bytes=4 * 2**20),
    )(gate, up, down, rows)


def body(
    shards,
    widths,
    w_gate,
    low_gate,
    high_gate,
    w_up,
    low_up,
    high_up,
    w_down,
    low_down,
    high_down,
    norm_train,
    norm_step,
):
    count = norm_train.shape[0]
    wide, tall = w_gate.shape
    if shards % X or wide % LANES or tall % (CUTS * LANES) or LANES % count or (shards * widths * count) % LANES:
        gate = merged(w_gate, low_gate, high_gate)
        up = merged(w_up, low_up, high_up)
        down = merged(w_down, low_down, high_down)
        gate, up, down = (
            lax.all_gather(gate, "shard", axis=0, tiled=True),
            lax.all_gather(up, "shard", axis=0, tiled=True),
            lax.all_gather(down, "shard", axis=1, tiled=True),
        )
        gain = (norm_train + norm_step).astype(jnp.bfloat16)
        gain = lax.all_gather(gain, ("shard", "width"), axis=0, tiled=True)
        return gate.T, up.T, down.T, gain
    args = (
        w_gate, low_gate.T, high_gate, w_up, low_up.T, high_up, w_down, low_down.T, high_down,
        norm_train.reshape(1, count), norm_step.reshape(1, count),
    )
    gate, up, down, rows = gather_all(shards, widths, args)
    per = LANES // count
    gate, up, down, norm = write_out(gate, up, down, rows.reshape(-1, per, LANES))
    return gate, up, down, norm.reshape(-1)


def solution(mesh):
    return jax.shard_map(
        functools.partial(body, mesh.shape["shard"], mesh.shape["width"]),
        mesh=mesh,
        in_specs=(
            P("shard", "width"),
            P("shard", None),
            P(None, "width"),
            P("shard", "width"),
            P("shard", None),
            P(None, "width"),
            P("width", "shard"),
            P("width", None),
            P(None, "shard"),
            P(("shard", "width")),
            P(("shard", "width")),
        ),
        out_specs=(P("width", None), P("width", None), P(None, "width"), P()),
        check_vma=False,
    )
```

```python
import functools

import jax
import jax.numpy as jnp
from jax import lax
from jax.experimental import pallas as pl
from jax.experimental.pallas import tpu as pltpu
from jax.sharding import PartitionSpec as P

mix_rate = 2.0
MESH = pl.DeviceIdType.MESH
X = 2
LANES = 128

UNITS = 16
LINE = ((0, 0, 1), (0, 1, 3), (0, 4, 12), (1, 0, 8), (2, 0, 8), (2, 8, 8))
PAIR = ((1, 8, 8),)
ORDER = LINE[:3] + PAIR + LINE[3:]
UP, DOWN, SIDE = 0, 1, 2
WAYS = 3
WRITES = 4


def units_of(pieces, t):
    return sum(n for array, _, n in pieces if array == t)


def merged(w, low, high):
    fresh = w.astype(jnp.float32) + mix_rate * jnp.dot(
        low, high, preferred_element_type=jnp.float32
    )
    return fresh.astype(jnp.bfloat16)


def when(cond, fn):
    if cond is None:
        fn()
    else:
        pl.when(cond)(fn)


def both(a, b):
    if a is None:
        return b
    if b is None:
        return a
    return jnp.logical_and(a, b)


def gather_kernel(
    shards, widths,
    w_gate, low_gate, high_gate, w_up, low_up, high_up, w_down, low_down, high_down, train, step,
    o_gate, o_up, o_down, o_norm,
    v_gate, v_up, v_down, v_low_gate, v_low_up, v_low_down, v_high_gate, v_high_up, v_high_down,
    v_train, v_step, l_gate, l_up, h_down,
    send_sem, line_sem, pair_sem, side_sem, norm_send, norm_recv, load_sem, small_sem,
):
    lines = shards // X
    me, w = lax.axis_index("shard"), lax.axis_index("width")
    z, x = me // X, me % X
    partner = z * X + (1 - x)
    outs = (o_gate, o_up, o_down)
    wide, tall = w_gate.shape
    unit = tall // UNITS

    head = LINE[0][2] * unit
    loads = [
        pltpu.make_async_copy(w_gate.at[:, pl.ds(0, head)], v_gate.at[:, pl.ds(0, head)], load_sem.at[0]),
        pltpu.make_async_copy(w_gate.at[:, pl.ds(head, tall - head)], v_gate.at[:, pl.ds(head, tall - head)], load_sem.at[1]),
        pltpu.make_async_copy(w_up, v_up, load_sem.at[2]),
        pltpu.make_async_copy(w_down, v_down, load_sem.at[3]),
    ]
    smalls = (
        (low_gate, v_low_gate), (high_gate, v_high_gate),
        (low_up, v_low_up), (high_up, v_high_up),
        (low_down, v_low_down), (high_down, v_high_down),
        (train, v_train), (step, v_step),
    )
    small = [pltpu.make_async_copy(a, b, small_sem.at[i]) for i, (a, b) in enumerate(smalls)]
    for copy in small[:2] + loads[:2] + small[2:4] + loads[2:3] + small[4:6] + loads[3:] + small[6:]:
        copy.start()

    def target(way):
        return {UP: me + X, DOWN: me - X, SIDE: partner}[way]

    def has(way):
        return {UP: z + 1 < lines, DOWN: z > 0, SIDE: None}[way]

    barrier = pltpu.get_barrier_semaphore()
    peers = [lax.rem(w + k, widths) for k in range(1, widths)]
    for way in (UP, DOWN, SIDE):
        when(
            has(way),
            lambda way=way: pl.semaphore_signal(
                barrier, inc=1, device_id=(target(way), w), device_id_type=MESH
            ),
        )
    for p in peers:
        pl.semaphore_signal(barrier, inc=1, device_id=(me, p), device_id_type=MESH)

    def place(s, c):
        t, first, n = c
        block = pl.ds(pl.multiple_of(s * wide, wide), wide)
        inner = pl.ds(first * unit, n * unit)
        return outs[t].at[inner, block] if t < 2 else outs[t].at[block, inner]

    def receipt(way, s, c):
        if c in PAIR:
            return pair_sem.at[s * len(PAIR) + PAIR.index(c)]
        return side_sem.at[c[0]] if way == SIDE else line_sem.at[s // X * len(LINE) + LINE.index(c)]

    def remote(way, s, c):
        return pltpu.make_async_remote_copy(
            src_ref=place(s, c),
            dst_ref=place(s, c),
            send_sem=send_sem.at[way * len(outs) + c[0]],
            recv_sem=receipt(way, s, c),
            device_id=(target(way), w),
            device_id_type=MESH,
        )

    def send(way, s, c, cond=None):
        when(both(cond, has(way)), lambda: remote(way, s, c).start())

    def arrive(way, s, c, cond=None):
        when(cond, lambda: remote(way, s, c).wait_recv())

    def bulk(t, elements):
        return outs[t].at[pl.ds(0, elements // outs[t].shape[1])]

    def drain(way, t, units):
        ref = bulk(t, units * unit * wide)
        pltpu.make_async_remote_copy(
            src_ref=ref, dst_ref=ref, send_sem=send_sem.at[way * len(outs) + t], recv_sem=side_sem.at[t],
            device_id=(partner, w), device_id_type=MESH,
        ).wait_send()

    def collect(t, units):
        ref = bulk(t, units * unit * wide)
        pltpu.make_async_remote_copy(
            src_ref=ref, dst_ref=ref, send_sem=send_sem.at[t], recv_sem=side_sem.at[t],
            device_id=(partner, w), device_id_type=MESH,
        ).wait_recv()

    waits = {LINE[0]: loads[:1], LINE[1]: loads[1:2]}
    seen = set()

    def compute(c):
        t, first, n = c
        pending = waits.get(c, [])
        if t not in seen:
            seen.add(t)
            pending = small[2 * t : 2 * t + 2] + (pending if t == 0 else loads[t + 1 : t + 2])
        for copy in pending:
            copy.wait()
        if len(pending) > 1:
            if t == 0:
                l_gate[...] = v_low_gate[...].T
            elif t == 1:
                l_up[...] = v_low_up[...].T
            else:
                h_down[...] = v_high_down[...].T
        columns = pl.ds(pl.multiple_of(me * wide, wide), wide)

        @pl.loop(0, n * unit // LANES)
        def _(i):
            at = pl.ds(pl.multiple_of(first * unit + i * LANES, LANES), LANES)
            if t < 2:
                block, low, high = ((v_gate, l_gate, v_high_gate), (v_up, l_up, v_high_up))[t]
                outs[t][at, columns] = merged(block[:, at], low[...], high[:, at]).T
            else:
                o_down[columns, at] = merged(v_down[at, :].T, h_down[...], v_low_down[:, at])

    compute(ORDER[0])
    inner = jnp.logical_and(z > 0, z + 1 < lines)
    pl.when(inner)(lambda: pl.semaphore_wait(barrier, widths + 2))
    ends = widths + (1 if lines > 1 else 0)
    pl.when(jnp.logical_not(inner))(lambda: pl.semaphore_wait(barrier, ends))
    for k, c in enumerate(ORDER):
        if k:
            compute(c)
        if c in LINE:
            send(UP, me, c)
            send(DOWN, me, c)
        send(SIDE, me, c)

    def norm_rows(begin, count):
        return o_norm.at[pl.ds(begin, count)]

    def norm_copy(begin, count, sem, rsem, dev):
        return pltpu.make_async_remote_copy(
            src_ref=norm_rows(begin, count), dst_ref=norm_rows(begin, count),
            send_sem=norm_send.at[sem], recv_sem=norm_recv.at[rsem],
            device_id=dev, device_id_type=MESH,
        )

    for copy in small[6:]:
        copy.wait()
    gain = v_train[...] + v_step[...]
    row = jnp.concatenate([gain] * (LANES // gain.shape[1]), axis=1)
    o_norm[pl.ds(me * widths + w, 1)] = row.reshape(1, 1, LANES)
    for p in peers:
        norm_copy(me * widths + w, 1, 3, 0, (me, p)).start()
    tiles = lambda: norm_copy(0, widths - 1, 3, 0, (partner, w))
    norm_side = lambda s: norm_copy(s * widths, widths, SIDE, 1, (partner, w))
    plane_rows = X * widths
    norm_plane = lambda way, plane: norm_copy(plane * plane_rows, plane_rows, way, 2 + plane, (target(way), w))
    if widths > 1:
        tiles().wait_recv()
    norm_side(me).start()

    def hops(d):
        return ((UP, z - d, z >= d), (DOWN, z + d, z + d < lines))

    def forward_line(d):
        for c in LINE:
            for way, plane, cond in hops(d):
                s = plane * X + x
                arrive(way, s, c, cond)
                send(way, s, c, cond)
                send(SIDE, s, c, cond)

    def forward_pair(d):
        if d == 0:
            for c in PAIR:
                send(UP, me, c)
                send(DOWN, me, c)
            norm_side(partner).wait_recv()
            for way in (UP, DOWN):
                when(has(way), lambda way=way: norm_plane(way, z).start())
            for c in PAIR:
                arrive(SIDE, partner, c)
                send(UP, partner, c)
                send(DOWN, partner, c)
            return
        for way, plane, cond in hops(d):
            when(cond, lambda way=way, plane=plane: norm_plane(way, plane).wait_recv())
            when(both(cond, has(way)), lambda way=way, plane=plane: norm_plane(way, plane).start())
        for c in PAIR:
            for j in range(X):
                for way, plane, cond in hops(d):
                    s = plane * X + (x + j) % X
                    arrive(way, s, c, cond)
                    send(way, s, c, cond)

    for d in range(1, lines):
        forward_line(d)
        forward_pair(d - 1)
    forward_pair(lines - 1)

    for t in range(len(outs)):
        collect(t, lines * units_of(LINE, t))
        drain(SIDE, t, lines * units_of(LINE, t) + units_of(PAIR, t))
    norm_side(me).wait_send()
    if widths > 1:
        tiles().wait_send()
    for way in (UP, DOWN):
        for k in range(lines):
            planes = k + 1 if way == UP else lines - k

            @pl.when(both(z == k, has(way)))
            def _(way=way, planes=planes):
                for t in range(len(outs)):
                    drain(way, t, planes * (units_of(LINE, t) + X * units_of(PAIR, t)))
                norm_copy(0, planes * plane_rows, way, 0, (partner, w)).wait_send()


def gather_all(shards, widths, args):
    lines = shards // X
    w_gate, low_gate, high_gate, w_up, low_up, high_up, w_down, low_down, high_down, train, step = args
    hbm = pl.BlockSpec(memory_space=pltpu.HBM)
    vmem = pl.BlockSpec(memory_space=pltpu.VMEM)
    like = lambda a: pltpu.VMEM(a.shape, a.dtype)
    flip = lambda a: pltpu.VMEM(a.shape[::-1], a.dtype)
    wide, tall = w_gate.shape
    full = pltpu.VMEM((tall, shards * wide), w_gate.dtype)
    return pl.pallas_call(
        functools.partial(gather_kernel, shards, widths),
        out_shape=(
            full, full,
            pltpu.VMEM((shards * wide, tall), w_down.dtype),
            pltpu.VMEM((shards * widths, 1, LANES), train.dtype),
        ),
        in_specs=[hbm] * len(args),
        out_specs=(vmem,) * 4,
        scratch_shapes=[
            like(w_gate), like(w_up), like(w_down),
            like(low_gate), like(low_up), like(low_down),
            like(high_gate), like(high_up), like(high_down),
            like(train), like(step),
            flip(low_gate), flip(low_up), flip(high_down),
            pltpu.SemaphoreType.DMA((WAYS * 3,)),
            pltpu.SemaphoreType.DMA((lines * len(LINE),)),
            pltpu.SemaphoreType.DMA((shards * len(PAIR),)),
            pltpu.SemaphoreType.DMA((3,)),
            pltpu.SemaphoreType.DMA((4,)),
            pltpu.SemaphoreType.DMA((2 + lines,)),
            pltpu.SemaphoreType.DMA((4,)),
            pltpu.SemaphoreType.DMA((8,)),
        ],
        compiler_params=pltpu.CompilerParams(collective_id=0, has_side_effects=True, vmem_limit_bytes=16 * 2**20),
    )(*(pltpu.with_memory_space_constraint(a, pltpu.HBM) for a in args))


def write_kernel(gate, up, down, rows, o_gate, o_up, o_down, o_norm, norm, sem):
    pairs = ((gate, o_gate), (up, o_up), (down, o_down))
    part = gate.shape[0] // WRITES
    copies = [
        pltpu.make_async_copy(a.at[pl.ds(j * part, part)], b.at[pl.ds(j * part, part)], sem.at[i * WRITES + j])
        for i, (a, b) in enumerate(pairs)
        for j in range(WRITES)
    ]
    for copy in copies:
        copy.start()
    per = rows.shape[1]
    lane = lax.broadcasted_iota(jnp.int32, norm.shape, 1) // (LANES // per)
    line = rows[:, 0, :]
    for j in range(1, per):
        line = jnp.where(lane == j, rows[:, j, :], line)
    norm[...] = line.astype(norm.dtype)
    last = pltpu.make_async_copy(norm, o_norm, sem.at[len(copies)])
    last.start()
    for copy in copies:
        copy.wait()
    last.wait()


def write_out(gate, up, down, rows):
    any_ = pl.BlockSpec(memory_space=pl.ANY)
    vmem = pl.BlockSpec(memory_space=pltpu.VMEM)
    norm = (rows.shape[0], LANES)
    return pl.pallas_call(
        write_kernel,
        out_shape=tuple(jax.ShapeDtypeStruct(a.shape, a.dtype) for a in (gate, up, down))
        + (jax.ShapeDtypeStruct(norm, jnp.bfloat16),),
        in_specs=[any_] * 3 + [vmem],
        out_specs=(any_,) * 4,
        scratch_shapes=[pltpu.VMEM(norm, jnp.bfloat16), pltpu.SemaphoreType.DMA((3 * WRITES + 1,))],
        compiler_params=pltpu.CompilerParams(vmem_limit_bytes=4 * 2**20),
    )(gate, up, down, rows)


def body(
    shards,
    widths,
    w_gate,
    low_gate,
    high_gate,
    w_up,
    low_up,
    high_up,
    w_down,
    low_down,
    high_down,
    norm_train,
    norm_step,
):
    count = norm_train.shape[0]
    wide, tall = w_gate.shape
    if shards % X or wide % LANES or tall % (UNITS * LANES) or LANES % count or (shards * widths * count) % LANES:
        gate = merged(w_gate, low_gate, high_gate)
        up = merged(w_up, low_up, high_up)
        down = merged(w_down, low_down, high_down)
        gate, up, down = (
            lax.all_gather(gate, "shard", axis=0, tiled=True),
            lax.all_gather(up, "shard", axis=0, tiled=True),
            lax.all_gather(down, "shard", axis=1, tiled=True),
        )
        gain = (norm_train + norm_step).astype(jnp.bfloat16)
        gain = lax.all_gather(gain, ("shard", "width"), axis=0, tiled=True)
        return gate.T, up.T, down.T, gain
    args = (
        w_gate, low_gate.T, high_gate, w_up, low_up.T, high_up, w_down, low_down.T, high_down,
        norm_train.reshape(1, count), norm_step.reshape(1, count),
    )
    gate, up, down, rows = gather_all(shards, widths, args)
    per = LANES // count
    gate, up, down, norm = write_out(gate, up, down, rows.reshape(-1, per, LANES))
    return gate, up, down, norm.reshape(-1)


def solution(mesh):
    return jax.shard_map(
        functools.partial(body, mesh.shape["shard"], mesh.shape["width"]),
        mesh=mesh,
        in_specs=(
            P("shard", "width"),
            P("shard", None),
            P(None, "width"),
            P("shard", "width"),
            P("shard", None),
            P(None, "width"),
            P("width", "shard"),
            P("width", None),
            P(None, "shard"),
            P(("shard", "width")),
            P(("shard", "width")),
        ),
        out_specs=(P("width", None), P("width", None), P(None, "width"), P()),
        check_vma=False,
    )
```

```python
import functools

import jax
import jax.numpy as jnp
from jax import lax
from jax.experimental import pallas as pl
from jax.experimental.pallas import tpu as pltpu
from jax.sharding import PartitionSpec as P

mix_rate = 2.0
MESH = pl.DeviceIdType.MESH
X = 2
LANES = 128

UNITS = 16
LINE = ((0, 0, 1), (0, 1, 3), (0, 4, 12), (1, 0, 8), (2, 0, 8), (2, 8, 3), (2, 11, 5))
PAIR = ((1, 8, 3), (1, 11, 5))
LATE_LINE, LATE_PAIR = LINE[-1], PAIR[-1]
ORDER = LINE[:3] + PAIR + LINE[3:]
UP, DOWN, SIDE = 0, 1, 2
WAYS = 3
WRITES = 4
WRITE_FLOPS = 2 * 10**9


def units_of(pieces, t):
    return sum(n for array, _, n in pieces if array == t)


def merged(w, low, high):
    fresh = w.astype(jnp.float32) + mix_rate * jnp.dot(
        low, high, preferred_element_type=jnp.float32
    )
    return fresh.astype(jnp.bfloat16)


def when(cond, fn):
    if cond is None:
        fn()
    else:
        pl.when(cond)(fn)


def both(a, b):
    if a is None:
        return b
    if b is None:
        return a
    return jnp.logical_and(a, b)


def far_plane(z, lines):
    return jnp.where(z < lines // 2, lines - 1, 0)


def gather_kernel(
    shards, widths,
    w_gate, low_gate, high_gate, w_up, low_up, high_up, w_down, low_down, high_down, train, step,
    o_gate, o_up, o_down, o_norm, late_x, late_z,
    v_gate, v_up, v_down, v_low_gate, v_low_up, v_low_down, v_high_gate, v_high_up, v_high_down,
    v_train, v_step, l_gate, l_up, h_down,
    send_sem, line_sem, pair_sem, side_sem, norm_send, norm_recv, load_sem, small_sem,
):
    lines = shards // X
    me, w = lax.axis_index("shard"), lax.axis_index("width")
    z, x = me // X, me % X
    partner = z * X + (1 - x)
    outs = (o_gate, o_up, o_down)
    wide, tall = w_gate.shape
    unit = tall // UNITS

    head = LINE[0][2] * unit
    loads = [
        pltpu.make_async_copy(w_gate.at[:, pl.ds(0, head)], v_gate.at[:, pl.ds(0, head)], load_sem.at[0]),
        pltpu.make_async_copy(w_gate.at[:, pl.ds(head, tall - head)], v_gate.at[:, pl.ds(head, tall - head)], load_sem.at[1]),
        pltpu.make_async_copy(w_up, v_up, load_sem.at[2]),
        pltpu.make_async_copy(w_down, v_down, load_sem.at[3]),
    ]
    smalls = (
        (low_gate, v_low_gate), (high_gate, v_high_gate),
        (low_up, v_low_up), (high_up, v_high_up),
        (low_down, v_low_down), (high_down, v_high_down),
        (train, v_train), (step, v_step),
    )
    small = [pltpu.make_async_copy(a, b, small_sem.at[i]) for i, (a, b) in enumerate(smalls)]
    for copy in small[:2] + loads[:2] + small[2:4] + loads[2:3] + small[4:6] + loads[3:] + small[6:]:
        copy.start()

    def target(way):
        return {UP: me + X, DOWN: me - X, SIDE: partner}[way]

    def has(way):
        return {UP: z + 1 < lines, DOWN: z > 0, SIDE: None}[way]

    barrier = pltpu.get_barrier_semaphore()
    peers = [lax.rem(w + k, widths) for k in range(1, widths)]
    for way in (UP, DOWN, SIDE):
        when(
            has(way),
            lambda way=way: pl.semaphore_signal(
                barrier, inc=1, device_id=(target(way), w), device_id_type=MESH
            ),
        )
    for p in peers:
        pl.semaphore_signal(barrier, inc=1, device_id=(me, p), device_id_type=MESH)

    def place(s, c):
        t, first, n = c
        block = pl.ds(pl.multiple_of(s * wide, wide), wide)
        inner = pl.ds(first * unit, n * unit)
        return outs[t].at[inner, block] if t < 2 else outs[t].at[block, inner]

    def receipt(way, s, c):
        if c in PAIR:
            return pair_sem.at[s * len(PAIR) + PAIR.index(c)]
        return side_sem.at[c[0]] if way == SIDE else line_sem.at[s // X * len(LINE) + LINE.index(c)]

    def remote(way, s, c):
        return pltpu.make_async_remote_copy(
            src_ref=place(s, c),
            dst_ref=place(s, c),
            send_sem=send_sem.at[way * len(outs) + c[0]],
            recv_sem=receipt(way, s, c),
            device_id=(target(way), w),
            device_id_type=MESH,
        )

    def send(way, s, c, cond=None):
        when(both(cond, has(way)), lambda: remote(way, s, c).start())

    def arrive(way, s, c, cond=None):
        when(cond, lambda: remote(way, s, c).wait_recv())

    def bulk(t, elements):
        return outs[t].at[pl.ds(0, elements // outs[t].shape[1])]

    def drain(way, t, units):
        ref = bulk(t, units * unit * wide)
        pltpu.make_async_remote_copy(
            src_ref=ref, dst_ref=ref, send_sem=send_sem.at[way * len(outs) + t], recv_sem=side_sem.at[t],
            device_id=(partner, w), device_id_type=MESH,
        ).wait_send()

    def collect(t, units):
        ref = bulk(t, units * unit * wide)
        pltpu.make_async_remote_copy(
            src_ref=ref, dst_ref=ref, send_sem=send_sem.at[t], recv_sem=side_sem.at[t],
            device_id=(partner, w), device_id_type=MESH,
        ).wait_recv()

    waits = {LINE[0]: loads[:1], LINE[1]: loads[1:2]}
    seen = set()

    def compute(c):
        t, first, n = c
        pending = waits.get(c, [])
        if t not in seen:
            seen.add(t)
            pending = small[2 * t : 2 * t + 2] + (pending if t == 0 else loads[t + 1 : t + 2])
        for copy in pending:
            copy.wait()
        if len(pending) > 1:
            if t == 0:
                l_gate[...] = v_low_gate[...].T
            elif t == 1:
                l_up[...] = v_low_up[...].T
            else:
                h_down[...] = v_high_down[...].T
        columns = pl.ds(pl.multiple_of(me * wide, wide), wide)

        @pl.loop(0, n * unit // LANES)
        def _(i):
            at = pl.ds(pl.multiple_of(first * unit + i * LANES, LANES), LANES)
            if t < 2:
                block, low, high = ((v_gate, l_gate, v_high_gate), (v_up, l_up, v_high_up))[t]
                outs[t][at, columns] = merged(block[:, at], low[...], high[:, at]).T
            else:
                o_down[columns, at] = merged(v_down[at, :].T, h_down[...], v_low_down[:, at])

    compute(ORDER[0])
    inner = jnp.logical_and(z > 0, z + 1 < lines)
    pl.when(inner)(lambda: pl.semaphore_wait(barrier, widths + 2))
    ends = widths + (1 if lines > 1 else 0)
    pl.when(jnp.logical_not(inner))(lambda: pl.semaphore_wait(barrier, ends))
    for k, c in enumerate(ORDER):
        if k:
            compute(c)
        if c in LINE:
            send(UP, me, c)
            send(DOWN, me, c)
        send(SIDE, me, c)

    def norm_rows(begin, count):
        return o_norm.at[pl.ds(begin, count)]

    def norm_copy(begin, count, sem, rsem, dev):
        return pltpu.make_async_remote_copy(
            src_ref=norm_rows(begin, count), dst_ref=norm_rows(begin, count),
            send_sem=norm_send.at[sem], recv_sem=norm_recv.at[rsem],
            device_id=dev, device_id_type=MESH,
        )

    for copy in small[6:]:
        copy.wait()
    gain = v_train[...] + v_step[...]
    row = jnp.concatenate([gain] * (LANES // gain.shape[1]), axis=1)
    o_norm[pl.ds(me * widths + w, 1)] = row.reshape(1, 1, LANES)
    for p in peers:
        norm_copy(me * widths + w, 1, 3, 0, (me, p)).start()
    tiles = lambda: norm_copy(0, widths - 1, 3, 0, (partner, w))
    norm_side = lambda s: norm_copy(s * widths, widths, SIDE, 1, (partner, w))
    plane_rows = X * widths
    norm_plane = lambda way, plane: norm_copy(plane * plane_rows, plane_rows, way, 2 + plane, (target(way), w))
    if widths > 1:
        tiles().wait_recv()
    norm_side(me).start()

    far = far_plane(z, lines)

    def hops(d):
        return ((UP, z - d, z >= d), (DOWN, z + d, z + d < lines))

    def forward_line(d):
        for c in LINE:
            for way, plane, cond in hops(d):
                s = plane * X + x
                arrive(way, s, c, cond)
                send(way, s, c, cond)
                send(SIDE, s, c, both(cond, plane != far) if c == LATE_LINE else cond)

    source = {UP: 0, DOWN: lines - 1}
    feeds = {UP: z == lines - 2, DOWN: z == 1}

    def send_pair(way, plane, j, c, cond=None):
        if c == LATE_PAIR and j == 1:
            late = jnp.logical_and(feeds[way], plane == source[way])
            cond = both(cond, jnp.logical_not(late))
        send(way, plane * X + (x + j) % X, c, cond)

    def arrive_pair(way, plane, j, c, cond):
        if c == LATE_PAIR and j == 1:
            end = {UP: z == lines - 1, DOWN: z == 0}[way]
            late = jnp.logical_and(end, plane == source[way])
            cond = both(cond, jnp.logical_not(late))
        arrive(way, plane * X + (x + j) % X, c, cond)

    def forward_pair(d):
        if d == 0:
            for c in PAIR:
                send(UP, me, c)
                send(DOWN, me, c)
            norm_side(partner).wait_recv()
            for way in (UP, DOWN):
                when(has(way), lambda way=way: norm_plane(way, z).start())
            for c in PAIR:
                arrive(SIDE, partner, c)
                send_pair(UP, z, 1, c)
                send_pair(DOWN, z, 1, c)
            return
        for way, plane, cond in hops(d):
            when(cond, lambda way=way, plane=plane: norm_plane(way, plane).wait_recv())
            when(both(cond, has(way)), lambda way=way, plane=plane: norm_plane(way, plane).start())
        for c in PAIR:
            for j in range(X):
                for way, plane, cond in hops(d):
                    arrive_pair(way, plane, j, c, cond)
                    send_pair(way, plane, j, c, cond)

    for d in range(1, lines):
        forward_line(d)
        forward_pair(d - 1)
    bridge = jnp.logical_or(z == 1, z == lines - 2)
    keep = jnp.where(z == 1, lines - 1, 0) * X + (1 - x)
    keep = jnp.where(bridge, keep, me)
    late_x[...] = place(far * X + x, LATE_LINE)[...]
    late_z[...] = place(keep, LATE_PAIR)[...]
    forward_pair(lines - 1)

    for t in range(len(outs)):
        skipped = LATE_LINE[2] * (t == LATE_LINE[0])
        collect(t, lines * units_of(LINE, t) - skipped)
        drain(SIDE, t, lines * units_of(LINE, t) + units_of(PAIR, t) - skipped)
    norm_side(me).wait_send()
    if widths > 1:
        tiles().wait_send()
    for way in (UP, DOWN):
        for k in range(lines):
            planes = k + 1 if way == UP else lines - k

            @pl.when(both(z == k, has(way)))
            def _(way=way, planes=planes):
                feeder = k == (lines - 2 if way == UP else 1)
                for t in range(len(outs)):
                    skipped = LATE_PAIR[2] * (feeder and t == LATE_PAIR[0])
                    drain(way, t, planes * (units_of(LINE, t) + X * units_of(PAIR, t)) - skipped)
                norm_copy(0, planes * plane_rows, way, 0, (partner, w)).wait_send()


def gather_all(shards, widths, args):
    lines = shards // X
    w_gate, low_gate, high_gate, w_up, low_up, high_up, w_down, low_down, high_down, train, step = args
    hbm = pl.BlockSpec(memory_space=pltpu.HBM)
    vmem = pl.BlockSpec(memory_space=pltpu.VMEM)
    like = lambda a: pltpu.VMEM(a.shape, a.dtype)
    flip = lambda a: pltpu.VMEM(a.shape[::-1], a.dtype)
    wide, tall = w_gate.shape
    full = pltpu.VMEM((tall, shards * wide), w_gate.dtype)
    return pl.pallas_call(
        functools.partial(gather_kernel, shards, widths),
        out_shape=(
            full, full,
            pltpu.VMEM((shards * wide, tall), w_down.dtype),
            pltpu.VMEM((shards * widths, 1, LANES), train.dtype),
            pltpu.VMEM((wide, LATE_LINE[2] * tall // UNITS), w_down.dtype),
            pltpu.VMEM((LATE_PAIR[2] * tall // UNITS, wide), w_up.dtype),
        ),
        in_specs=[hbm] * len(args),
        out_specs=(vmem,) * 6,
        scratch_shapes=[
            like(w_gate), like(w_up), like(w_down),
            like(low_gate), like(low_up), like(low_down),
            like(high_gate), like(high_up), like(high_down),
            like(train), like(step),
            flip(low_gate), flip(low_up), flip(high_down),
            pltpu.SemaphoreType.DMA((WAYS * 3,)),
            pltpu.SemaphoreType.DMA((lines * len(LINE),)),
            pltpu.SemaphoreType.DMA((shards * len(PAIR),)),
            pltpu.SemaphoreType.DMA((3,)),
            pltpu.SemaphoreType.DMA((4,)),
            pltpu.SemaphoreType.DMA((2 + lines,)),
            pltpu.SemaphoreType.DMA((4,)),
            pltpu.SemaphoreType.DMA((8,)),
        ],
        compiler_params=pltpu.CompilerParams(collective_id=0, has_side_effects=True, vmem_limit_bytes=16 * 2**20),
    )(*(pltpu.with_memory_space_constraint(a, pltpu.HBM) for a in args))


def write_kernel(gate, up, down, rows, o_gate, o_up, o_down, o_norm, norm, sem):
    pairs = ((gate, o_gate), (up, o_up), (down, o_down))
    part = gate.shape[0] // WRITES
    copies = [
        pltpu.make_async_copy(a.at[pl.ds(j * part, part)], b.at[pl.ds(j * part, part)], sem.at[i * WRITES + j])
        for i, (a, b) in enumerate(pairs)
        for j in range(WRITES)
    ]
    for copy in copies:
        copy.start()
    per = rows.shape[1]
    lane = lax.broadcasted_iota(jnp.int32, norm.shape, 1) // (LANES // per)
    line = rows[:, 0, :]
    for j in range(1, per):
        line = jnp.where(lane == j, rows[:, j, :], line)
    norm[...] = line.astype(norm.dtype)
    last = pltpu.make_async_copy(norm, o_norm, sem.at[len(copies)])
    last.start()
    for copy in copies:
        copy.wait()
    last.wait()


def write_out(gate, up, down, rows):
    any_ = pl.BlockSpec(memory_space=pl.ANY)
    vmem = pl.BlockSpec(memory_space=pltpu.VMEM)
    norm = (rows.shape[0], LANES)
    return pl.pallas_call(
        write_kernel,
        out_shape=tuple(jax.ShapeDtypeStruct(a.shape, a.dtype) for a in (gate, up, down))
        + (jax.ShapeDtypeStruct(norm, jnp.bfloat16),),
        in_specs=[any_] * 3 + [vmem],
        out_specs=(any_,) * 4,
        scratch_shapes=[pltpu.VMEM(norm, jnp.bfloat16), pltpu.SemaphoreType.DMA((3 * WRITES + 1,))],
        cost_estimate=pl.CostEstimate(flops=WRITE_FLOPS, bytes_accessed=2 * 3 * gate.size * 2, transcendentals=0),
        compiler_params=pltpu.CompilerParams(vmem_limit_bytes=4 * 2**20),
    )(gate, up, down, rows)


def late_kernel(lines, up, down, late_x, late_z, o_up, o_down, v_x, v_z, sem):
    me = lax.axis_index("shard")
    z, x = me // X, me % X
    wide, tall = late_z.shape[1], up.shape[0]
    unit = tall // UNITS
    end = jnp.logical_or(z == 0, z == lines - 1)
    block = (far_plane(z, lines) * X + (1 - x)) * wide
    block = pl.ds(pl.multiple_of(block, wide), wide)
    inner = lambda c: pl.ds(c[1] * unit, c[2] * unit)
    get_x = pltpu.make_async_copy(late_x, v_x, sem.at[0])
    get_z = pltpu.make_async_copy(late_z, v_z, sem.at[1])
    put_x = pltpu.make_async_copy(v_x, o_down.at[block, inner(LATE_LINE)], sem.at[2])
    put_z = pltpu.make_async_copy(v_z, o_up.at[inner(LATE_PAIR), block], sem.at[3])
    get_x.start()
    pl.when(end)(get_z.start)
    get_x.wait()
    put_x.start()

    @pl.when(end)
    def _():
        get_z.wait()
        put_z.start()
        put_z.wait()

    put_x.wait()


def write_late(lines, up, down, late_x, late_z):
    any_ = pl.BlockSpec(memory_space=pl.ANY)
    return pl.pallas_call(
        functools.partial(late_kernel, lines),
        out_shape=tuple(jax.ShapeDtypeStruct(a.shape, a.dtype) for a in (up, down)),
        in_specs=[any_] * 4,
        out_specs=(any_,) * 2,
        input_output_aliases={0: 0, 1: 1},
        scratch_shapes=[
            pltpu.VMEM(late_x.shape, late_x.dtype),
            pltpu.VMEM(late_z.shape, late_z.dtype),
            pltpu.SemaphoreType.DMA((4,)),
        ],
        compiler_params=pltpu.CompilerParams(vmem_limit_bytes=4 * 2**20),
    )(up, down, late_x, late_z)


def body(
    shards,
    widths,
    w_gate,
    low_gate,
    high_gate,
    w_up,
    low_up,
    high_up,
    w_down,
    low_down,
    high_down,
    norm_train,
    norm_step,
):
    count = norm_train.shape[0]
    wide, tall = w_gate.shape
    if shards % (2 * X) or wide % LANES or tall % (UNITS * LANES) or LANES % count or (shards * widths * count) % LANES:
        gate = merged(w_gate, low_gate, high_gate)
        up = merged(w_up, low_up, high_up)
        down = merged(w_down, low_down, high_down)
        gate, up, down = (
            lax.all_gather(gate, "shard", axis=0, tiled=True),
            lax.all_gather(up, "shard", axis=0, tiled=True),
            lax.all_gather(down, "shard", axis=1, tiled=True),
        )
        gain = (norm_train + norm_step).astype(jnp.bfloat16)
        gain = lax.all_gather(gain, ("shard", "width"), axis=0, tiled=True)
        return gate.T, up.T, down.T, gain
    args = (
        w_gate, low_gate.T, high_gate, w_up, low_up.T, high_up, w_down, low_down.T, high_down,
        norm_train.reshape(1, count), norm_step.reshape(1, count),
    )
    gate, up, down, rows, late_x, late_z = gather_all(shards, widths, args)
    per = LANES // count
    late_x = lax.ppermute(late_x, "shard", [(s, s ^ 1) for s in range(shards)])
    late_z = lax.ppermute(late_z, "shard", [(s, s ^ X) for s in range(shards)])
    gate, up, down, norm = write_out(gate, up, down, rows.reshape(-1, per, LANES))
    up, down = write_late(shards // X, up, down, late_x, late_z)
    return gate, up, down, norm.reshape(-1)


def solution(mesh):
    return jax.shard_map(
        functools.partial(body, mesh.shape["shard"], mesh.shape["width"]),
        mesh=mesh,
        in_specs=(
            P("shard", "width"),
            P("shard", None),
            P(None, "width"),
            P("shard", "width"),
            P("shard", None),
            P(None, "width"),
            P("width", "shard"),
            P("width", None),
            P(None, "shard"),
            P(("shard", "width")),
            P(("shard", "width")),
        ),
        out_specs=(P("width", None), P("width", None), P(None, "width"), P()),
        check_vma=False,
    )
```

```python
import functools

import jax
import jax.numpy as jnp
from jax import lax
from jax.experimental import pallas as pl
from jax.experimental.pallas import tpu as pltpu
from jax.sharding import PartitionSpec as P

mix_rate = 2.0
MESH = pl.DeviceIdType.MESH
X = 2
LANES = 128

UNITS = 16
LINE = ((0, 0, 16), (1, 0, 8), (2, 0, 10), (2, 10, 6))
PAIR = ((1, 8, 2), (1, 10, 6))
WHOLE = (1, 8, 8)
LATE_LINE, LATE_PAIR = LINE[-1], PAIR[-1]
ORDER = (
    ((0, 0, 1), LINE[0]), ((0, 1, 3), LINE[0]), ((0, 4, 12), LINE[0]),
    (PAIR[0], PAIR[0]), (PAIR[1], PAIR[1]),
    (LINE[1], LINE[1]), (LINE[2], LINE[2]), (LINE[3], LINE[3]),
)
UP, DOWN, SIDE = 0, 1, 2
WIDE = DOWN
WAYS = 3
WRITES = 4
WRITE_FLOPS = 2 * 10**9


def units_of(pieces, t):
    return sum(n for array, _, n in pieces if array == t)


def merged(w, low, high):
    fresh = w.astype(jnp.float32) + mix_rate * jnp.dot(
        low, high, preferred_element_type=jnp.float32
    )
    return fresh.astype(jnp.bfloat16)


def when(cond, fn):
    if cond is None:
        fn()
    else:
        pl.when(cond)(fn)


def both(a, b):
    if a is None:
        return b
    if b is None:
        return a
    return jnp.logical_and(a, b)


def far_plane(z, lines):
    return jnp.where(z < lines // 2, lines - 1, 0)


def gather_kernel(
    shards, widths,
    w_gate, low_gate, high_gate, w_up, low_up, high_up, w_down, low_down, high_down, train, step,
    o_gate, o_up, o_down, o_norm, late_x, late_z,
    v_gate, v_up, v_down, v_low_gate, v_low_up, v_low_down, v_high_gate, v_high_up, v_high_down,
    v_train, v_step, l_gate, l_up, h_down,
    send_sem, line_sem, pair_sem, side_sem, norm_send, norm_recv, load_sem, small_sem, extra_sem, ready,
):
    lines = shards // X
    me, w = lax.axis_index("shard"), lax.axis_index("width")
    z, x = me // X, me % X
    partner = z * X + (1 - x)
    outs = (o_gate, o_up, o_down)
    wide, tall = w_gate.shape
    unit = tall // UNITS

    head = ORDER[0][0][2] * unit
    loads = [
        pltpu.make_async_copy(w_gate.at[:, pl.ds(0, head)], v_gate.at[:, pl.ds(0, head)], load_sem.at[0]),
        pltpu.make_async_copy(w_gate.at[:, pl.ds(head, tall - head)], v_gate.at[:, pl.ds(head, tall - head)], load_sem.at[1]),
        pltpu.make_async_copy(w_up, v_up, load_sem.at[2]),
        pltpu.make_async_copy(w_down, v_down, load_sem.at[3]),
    ]
    smalls = (
        (low_gate, v_low_gate), (high_gate, v_high_gate),
        (low_up, v_low_up), (high_up, v_high_up),
        (low_down, v_low_down), (high_down, v_high_down),
        (train, v_train), (step, v_step),
    )
    small = [pltpu.make_async_copy(a, b, small_sem.at[i]) for i, (a, b) in enumerate(smalls)]
    for copy in small[:2] + loads[:2] + small[2:4] + loads[2:3] + small[4:6] + loads[3:] + small[6:]:
        copy.start()

    def target(way):
        return {UP: me + X, DOWN: me - X, SIDE: partner}[way]

    def has(way):
        return {UP: z + 1 < lines, DOWN: z > 0, SIDE: None}[way]

    barrier = pltpu.get_barrier_semaphore()
    peers = [lax.rem(w + k, widths) for k in range(1, widths)]
    after = [w + k < widths for k in range(1, widths)]

    def signal(sem, dev):
        pl.semaphore_signal(sem, inc=1, device_id=dev, device_id_type=MESH)

    when(has(UP), lambda: signal(barrier, (target(UP), w)))
    pl.when(x == 0)(lambda: signal(barrier, (partner, w)))
    for p, later in zip(peers, after):
        pl.when(later)(lambda p=p: signal(barrier, (me, p)))

    def enter():
        before = jnp.where(z > 0, 1, 0) + x + w
        pl.when(before > 0)(lambda: pl.semaphore_wait(barrier, before))
        when(has(DOWN), lambda: signal(ready.at[UP], (target(DOWN), w)))
        pl.when(x == 1)(lambda: signal(ready.at[SIDE], (partner, w)))
        for p, later in zip(peers, after):
            pl.when(jnp.logical_not(later))(lambda p=p: signal(ready.at[WIDE], (me, p)))

    def place(s, c):
        t, first, n = c
        block = pl.ds(pl.multiple_of(s * wide, wide), wide)
        inner = pl.ds(first * unit, n * unit)
        return outs[t].at[inner, block] if t < 2 else outs[t].at[block, inner]

    def receipt(way, s, whole, extra):
        if whole == WHOLE:
            return pair_sem.at[s // X * 3]
        if whole in PAIR:
            return pair_sem.at[s // X * 3 + 1 + PAIR.index(whole)]
        if extra:
            return extra_sem.at[0 if way == SIDE else 1]
        return side_sem.at[whole[0]] if way == SIDE else line_sem.at[s // X * len(LINE) + LINE.index(whole)]

    def remote(way, s, c, whole, extra=False):
        return pltpu.make_async_remote_copy(
            src_ref=place(s, c),
            dst_ref=place(s, c),
            send_sem=send_sem.at[way * len(outs) + c[0]],
            recv_sem=receipt(way, s, whole, extra),
            device_id=(target(way), w),
            device_id_type=MESH,
        )

    def send(way, s, c, cond=None, whole=None, extra=False):
        when(both(cond, has(way)), lambda: remote(way, s, c, whole or c, extra).start())

    def arrive(way, s, c, cond=None, extra=False):
        when(cond, lambda: remote(way, s, c, c, extra).wait_recv())

    def bulk(t, elements):
        return outs[t].at[pl.ds(0, elements // outs[t].shape[1])]

    def drain(way, t, units):
        ref = bulk(t, units * unit * wide)
        pltpu.make_async_remote_copy(
            src_ref=ref, dst_ref=ref, send_sem=send_sem.at[way * len(outs) + t], recv_sem=side_sem.at[t],
            device_id=(partner, w), device_id_type=MESH,
        ).wait_send()

    def collect(t, units):
        ref = bulk(t, units * unit * wide)
        pltpu.make_async_remote_copy(
            src_ref=ref, dst_ref=ref, send_sem=send_sem.at[t], recv_sem=side_sem.at[t],
            device_id=(partner, w), device_id_type=MESH,
        ).wait_recv()

    waits = {ORDER[0][0]: loads[:1], ORDER[1][0]: loads[1:2]}
    seen = set()

    def compute(c):
        t, first, n = c
        pending = waits.get(c, [])
        if t not in seen:
            seen.add(t)
            pending = small[2 * t : 2 * t + 2] + (pending if t == 0 else loads[t + 1 : t + 2])
        for copy in pending:
            copy.wait()
        if len(pending) > 1:
            if t == 0:
                l_gate[...] = v_low_gate[...].T
            elif t == 1:
                l_up[...] = v_low_up[...].T
            else:
                h_down[...] = v_high_down[...].T
        columns = pl.ds(pl.multiple_of(me * wide, wide), wide)

        @pl.loop(0, n * unit // LANES)
        def _(i):
            at = pl.ds(pl.multiple_of(first * unit + i * LANES, LANES), LANES)
            if t < 2:
                block, low, high = ((v_gate, l_gate, v_high_gate), (v_up, l_up, v_high_up))[t]
                outs[t][at, columns] = merged(block[:, at], low[...], high[:, at]).T
            else:
                o_down[columns, at] = merged(v_down[at, :].T, h_down[...], v_low_down[:, at])

    def send_up(c, whole):
        if whole in LINE:
            send(UP, me, c, None, whole)

    for k, (c, whole) in enumerate(ORDER):
        compute(c)
        if k == 0:
            enter()
        if k == 1:
            when(has(UP), lambda: pl.semaphore_wait(ready.at[UP], 1))
            send_up(*ORDER[0])
        if whole in LINE:
            send(DOWN, me, c, None, whole)
        if k == 0:
            pl.when(x == 0)(lambda: pl.semaphore_wait(ready.at[SIDE], 1))
        else:
            send_up(c, whole)
        send(SIDE, me, c, None, whole, c == LATE_LINE)

    def norm_rows(begin, count):
        return o_norm.at[pl.ds(begin, count)]

    def norm_copy(begin, count, sem, rsem, dev):
        return pltpu.make_async_remote_copy(
            src_ref=norm_rows(begin, count), dst_ref=norm_rows(begin, count),
            send_sem=norm_send.at[sem], recv_sem=norm_recv.at[rsem],
            device_id=dev, device_id_type=MESH,
        )

    for copy in small[6:]:
        copy.wait()
    gain = v_train[...] + v_step[...]
    row = jnp.concatenate([gain] * (LANES // gain.shape[1]), axis=1)
    o_norm[pl.ds(me * widths + w, 1)] = row.reshape(1, 1, LANES)
    pl.when(w + 1 < widths)(lambda: pl.semaphore_wait(ready.at[WIDE], widths - 1 - w))
    for p in peers:
        norm_copy(me * widths + w, 1, 3, 0, (me, p)).start()
    tiles = lambda: norm_copy(0, widths - 1, 3, 0, (partner, w))
    norm_side = lambda s: norm_copy(s * widths, widths, SIDE, 1, (partner, w))
    plane_rows = X * widths
    norm_plane = lambda way, plane: norm_copy(plane * plane_rows, plane_rows, way, 2 + plane, (target(way), w))
    if widths > 1:
        tiles().wait_recv()
    norm_side(me).start()

    far = far_plane(z, lines)
    inner = jnp.logical_and(z > 0, z + 1 < lines)
    lower = z < lines // 2
    mate = jnp.where(lower, z + 1, z - 1)
    lends = {
        DOWN: jnp.logical_and(z >= 2, z - 1 < lines // 2),
        UP: jnp.logical_and(z + 1 >= lines // 2, z + 2 < lines),
    }

    def by_side(plane):
        return jnp.logical_and(plane != far, jnp.logical_not(jnp.logical_and(inner, plane == mate)))

    def lend():
        arrive(SIDE, partner, LATE_LINE, None, True)
        for way in (UP, DOWN):
            send(way, partner, LATE_LINE, lends[way], None, True)

    def hops(d):
        return ((UP, z - d, z >= d), (DOWN, z + d, z + d < lines))

    def forward_line(d):
        for c in LINE:
            for way, plane, cond in hops(d):
                s = plane * X + x
                arrive(way, s, c, cond)
                send(way, s, c, cond)
                send(SIDE, s, c, both(cond, by_side(plane)) if c == LATE_LINE else cond)

    source = {UP: 0, DOWN: lines - 1}
    feeds = {UP: z == lines - 2, DOWN: z == 1}

    def send_pair(way, plane, j, c, cond=None):
        if c == LATE_PAIR:
            late = jnp.logical_and(feeds[way], plane == source[way])
            cond = both(cond, jnp.logical_not(late))
        send(way, plane * X + (x + j) % X, c, cond)

    def arrive_pair(way, plane, j, c, cond):
        if c == LATE_PAIR:
            end = {UP: z == lines - 1, DOWN: z == 0}[way]
            late = jnp.logical_and(end, plane == source[way])
            cond = both(cond, jnp.logical_not(late))
        arrive(way, plane * X + (x + j) % X, c, cond)

    def forward_pair(d):
        if d == 0:
            send(UP, me, WHOLE)
            send(DOWN, me, WHOLE)
            norm_side(partner).wait_recv()
            for way in (UP, DOWN):
                when(has(way), lambda way=way: norm_plane(way, z).start())
            for c in PAIR:
                arrive(SIDE, partner, c)
                send_pair(UP, z, 1, c)
                send_pair(DOWN, z, 1, c)
            return
        for way, plane, cond in hops(d):
            when(cond, lambda way=way, plane=plane: norm_plane(way, plane).wait_recv())
            when(both(cond, has(way)), lambda way=way, plane=plane: norm_plane(way, plane).start())
        for j, pieces in enumerate(((WHOLE,), PAIR)):
            for c in pieces:
                for way, plane, cond in hops(d):
                    arrive_pair(way, plane, j, c, cond)
                    send_pair(way, plane, j, c, cond)

    for d in range(1, lines):
        forward_line(d)
        forward_pair(d - 1)
        if d == 1:
            lend()
    bridge = jnp.logical_or(z == 1, z == lines - 2)
    keep = jnp.where(z == 1, lines - 1, 0) * X + (1 - x)
    keep = jnp.where(bridge, keep, me)
    late_x[...] = place(far * X + x, LATE_LINE)[...]
    late_z[...] = place(keep, LATE_PAIR)[...]
    forward_pair(lines - 1)

    arrive(DOWN, mate * X + 1 - x, LATE_LINE, inner, True)
    for t in range(len(outs)):
        if t != LATE_LINE[0]:
            collect(t, lines * units_of(LINE, t))
            drain(SIDE, t, lines * units_of(LINE, t) + units_of(PAIR, t))
            continue
        for cond, skipped in ((inner, 2 * LATE_LINE[2]), (jnp.logical_not(inner), LATE_LINE[2])):

            @pl.when(cond)
            def _(t=t, skipped=skipped):
                units = lines * units_of(LINE, t)
                collect(t, units - skipped - LATE_LINE[2])
                drain(SIDE, t, units + units_of(PAIR, t) - skipped)
    norm_side(me).wait_send()
    if widths > 1:
        tiles().wait_send()
    for way in (UP, DOWN):
        for k in range(lines):
            planes = k + 1 if way == UP else lines - k

            @pl.when(both(z == k, has(way)))
            def _(way=way, planes=planes):
                feeder = k == (lines - 2 if way == UP else 1)
                for t in range(len(outs)):
                    skipped = LATE_PAIR[2] * (feeder and t == LATE_PAIR[0])
                    lent = (k >= 2 and k - 1 < lines // 2) if way == DOWN else (k + 1 >= lines // 2 and k + 2 < lines)
                    lent = LATE_LINE[2] * (lent and t == LATE_LINE[0])
                    drain(way, t, planes * (units_of(LINE, t) + X * units_of(PAIR, t)) - skipped + lent)
                norm_copy(0, planes * plane_rows, way, 0, (partner, w)).wait_send()


def gather_all(shards, widths, args):
    lines = shards // X
    w_gate, low_gate, high_gate, w_up, low_up, high_up, w_down, low_down, high_down, train, step = args
    hbm = pl.BlockSpec(memory_space=pltpu.HBM)
    vmem = pl.BlockSpec(memory_space=pltpu.VMEM)
    like = lambda a: pltpu.VMEM(a.shape, a.dtype)
    flip = lambda a: pltpu.VMEM(a.shape[::-1], a.dtype)
    wide, tall = w_gate.shape
    full = pltpu.VMEM((tall, shards * wide), w_gate.dtype)
    return pl.pallas_call(
        functools.partial(gather_kernel, shards, widths),
        out_shape=(
            full, full,
            pltpu.VMEM((shards * wide, tall), w_down.dtype),
            pltpu.VMEM((shards * widths, 1, LANES), train.dtype),
            pltpu.VMEM((wide, LATE_LINE[2] * tall // UNITS), w_down.dtype),
            pltpu.VMEM((LATE_PAIR[2] * tall // UNITS, wide), w_up.dtype),
        ),
        in_specs=[hbm] * len(args),
        out_specs=(vmem,) * 6,
        scratch_shapes=[
            like(w_gate), like(w_up), like(w_down),
            like(low_gate), like(low_up), like(low_down),
            like(high_gate), like(high_up), like(high_down),
            like(train), like(step),
            flip(low_gate), flip(low_up), flip(high_down),
            pltpu.SemaphoreType.DMA((WAYS * 3,)),
            pltpu.SemaphoreType.DMA((lines * len(LINE),)),
            pltpu.SemaphoreType.DMA((lines * 3,)),
            pltpu.SemaphoreType.DMA((3,)),
            pltpu.SemaphoreType.DMA((4,)),
            pltpu.SemaphoreType.DMA((2 + lines,)),
            pltpu.SemaphoreType.DMA((4,)),
            pltpu.SemaphoreType.DMA((8,)),
            pltpu.SemaphoreType.DMA((2,)),
            pltpu.SemaphoreType.REGULAR((3,)),
        ],
        compiler_params=pltpu.CompilerParams(collective_id=0, has_side_effects=True, vmem_limit_bytes=16 * 2**20),
    )(*(pltpu.with_memory_space_constraint(a, pltpu.HBM) for a in args))


def write_kernel(gate, up, down, rows, o_gate, o_up, o_down, o_norm, norm, sem):
    pairs = ((gate, o_gate), (up, o_up), (down, o_down))
    part = gate.shape[0] // WRITES
    copies = [
        pltpu.make_async_copy(a.at[pl.ds(j * part, part)], b.at[pl.ds(j * part, part)], sem.at[i * WRITES + j])
        for i, (a, b) in enumerate(pairs)
        for j in range(WRITES)
    ]
    for copy in copies:
        copy.start()
    per = rows.shape[1]
    lane = lax.broadcasted_iota(jnp.int32, norm.shape, 1) // (LANES // per)
    line = rows[:, 0, :]
    for j in range(1, per):
        line = jnp.where(lane == j, rows[:, j, :], line)
    norm[...] = line.astype(norm.dtype)
    last = pltpu.make_async_copy(norm, o_norm, sem.at[len(copies)])
    last.start()
    for copy in copies:
        copy.wait()
    last.wait()


def write_out(gate, up, down, rows):
    any_ = pl.BlockSpec(memory_space=pl.ANY)
    vmem = pl.BlockSpec(memory_space=pltpu.VMEM)
    norm = (rows.shape[0], LANES)
    return pl.pallas_call(
        write_kernel,
        out_shape=tuple(jax.ShapeDtypeStruct(a.shape, a.dtype) for a in (gate, up, down))
        + (jax.ShapeDtypeStruct(norm, jnp.bfloat16),),
        in_specs=[any_] * 3 + [vmem],
        out_specs=(any_,) * 4,
        scratch_shapes=[pltpu.VMEM(norm, jnp.bfloat16), pltpu.SemaphoreType.DMA((3 * WRITES + 1,))],
        cost_estimate=pl.CostEstimate(flops=WRITE_FLOPS, bytes_accessed=2 * 3 * gate.size * 2, transcendentals=0),
        compiler_params=pltpu.CompilerParams(vmem_limit_bytes=4 * 2**20),
    )(gate, up, down, rows)


def late_kernel(lines, up, down, late_z, late_x, o_up, o_down, sem):
    me = lax.axis_index("shard")
    z, x = me // X, me % X
    wide, tall = late_z.shape[1], up.shape[0]
    unit = tall // UNITS
    end = jnp.logical_or(z == 0, z == lines - 1)
    block = (far_plane(z, lines) * X + (1 - x)) * wide
    block = pl.ds(pl.multiple_of(block, wide), wide)
    inner = lambda c: pl.ds(c[1] * unit, c[2] * unit)
    put_x = pltpu.make_async_copy(late_x, o_down.at[block, inner(LATE_LINE)], sem.at[0])
    put_z = pltpu.make_async_copy(late_z, o_up.at[inner(LATE_PAIR), block], sem.at[1])
    put_x.start()
    pl.when(end)(put_z.start)
    put_x.wait()
    pl.when(end)(put_z.wait)


def write_late(lines, up, down, late_x, late_z):
    any_ = pl.BlockSpec(memory_space=pl.ANY)
    vmem = pl.BlockSpec(memory_space=pltpu.VMEM)
    return pl.pallas_call(
        functools.partial(late_kernel, lines),
        out_shape=tuple(jax.ShapeDtypeStruct(a.shape, a.dtype) for a in (up, down)),
        in_specs=[any_] * 2 + [vmem] * 2,
        out_specs=(any_,) * 2,
        input_output_aliases={0: 0, 1: 1},
        scratch_shapes=[pltpu.SemaphoreType.DMA((2,))],
        compiler_params=pltpu.CompilerParams(vmem_limit_bytes=4 * 2**20),
    )(up, down, late_z, late_x)


def body(
    shards,
    widths,
    w_gate,
    low_gate,
    high_gate,
    w_up,
    low_up,
    high_up,
    w_down,
    low_down,
    high_down,
    norm_train,
    norm_step,
):
    count = norm_train.shape[0]
    wide, tall = w_gate.shape
    if shards % (2 * X) or wide % LANES or tall % (UNITS * LANES) or LANES % count or (shards * widths * count) % LANES:
        gate = merged(w_gate, low_gate, high_gate)
        up = merged(w_up, low_up, high_up)
        down = merged(w_down, low_down, high_down)
        gate, up, down = (
            lax.all_gather(gate, "shard", axis=0, tiled=True),
            lax.all_gather(up, "shard", axis=0, tiled=True),
            lax.all_gather(down, "shard", axis=1, tiled=True),
        )
        gain = (norm_train + norm_step).astype(jnp.bfloat16)
        gain = lax.all_gather(gain, ("shard", "width"), axis=0, tiled=True)
        return gate.T, up.T, down.T, gain
    args = (
        w_gate, low_gate.T, high_gate, w_up, low_up.T, high_up, w_down, low_down.T, high_down,
        norm_train.reshape(1, count), norm_step.reshape(1, count),
    )
    gate, up, down, rows, late_x, late_z = gather_all(shards, widths, args)
    per = LANES // count
    late_z = lax.ppermute(late_z, "shard", [(s, s ^ X) for s in range(shards)])
    late_x = lax.ppermute(late_x, "shard", [(s, s ^ 1) for s in range(shards)])
    gate, up, down, norm = write_out(gate, up, down, rows.reshape(-1, per, LANES))
    up, down = write_late(shards // X, up, down, late_x, late_z)
    return gate, up, down, norm.reshape(-1)


def solution(mesh):
    return jax.shard_map(
        functools.partial(body, mesh.shape["shard"], mesh.shape["width"]),
        mesh=mesh,
        in_specs=(
            P("shard", "width"),
            P("shard", None),
            P(None, "width"),
            P("shard", "width"),
            P("shard", None),
            P(None, "width"),
            P("width", "shard"),
            P("width", None),
            P(None, "shard"),
            P(("shard", "width")),
            P(("shard", "width")),
        ),
        out_specs=(P("width", None), P("width", None), P(None, "width"), P()),
        check_vma=False,
    )
```

```python
import functools
import math

import jax
import jax.numpy as jnp
from jax import lax
from jax.experimental import pallas as pl
from jax.experimental.pallas import tpu as pltpu
from jax.sharding import PartitionSpec as P

mix_rate = 2.0
MESH = pl.DeviceIdType.MESH
X = 2
LANES = 128

UNITS = 16
LINE = ((0, 0, 16), (1, 0, 8), (2, 0, 10), (2, 10, 6))
PAIR = ((1, 8, 2), (1, 10, 6))
WHOLE = (1, 8, 8)
BUNDLES = (LINE[:1], LINE[1:3], LINE[3:])
LATE_LINE, LATE_PAIR = LINE[-1], PAIR[-1]
ORDER = (
    ((0, 0, 1), LINE[0]), ((0, 1, 3), LINE[0]), ((0, 4, 12), LINE[0]),
    (PAIR[0], PAIR[0]), (PAIR[1], PAIR[1]),
    (LINE[1], LINE[1]), (LINE[2], LINE[2]), (LINE[3], LINE[3]),
)
UP, DOWN, SIDE = 0, 1, 2
WIDE = DOWN
WAYS = 3
WRITES = 4
WRITE_FLOPS = 2 * 10**9


def units_of(pieces, arrays=(0, 1, 2)):
    return sum(n for array, _, n in pieces if array in arrays)


SHARES = ((0, 1), (2,))


def merged(w, low, high):
    fresh = w.astype(jnp.float32) + mix_rate * jnp.dot(
        low, high, preferred_element_type=jnp.float32
    )
    return fresh.astype(jnp.bfloat16)


def when(cond, fn):
    if cond is None:
        fn()
    else:
        pl.when(cond)(fn)


def both(a, b):
    if a is None:
        return b
    if b is None:
        return a
    return jnp.logical_and(a, b)


def far_plane(z, lines):
    return jnp.where(z < lines // 2, lines - 1, 0)


def gather_kernel(
    shards, widths,
    w_gate, low_gate, high_gate, w_up, low_up, high_up, w_down, low_down, high_down, train, step,
    o_gate, o_up, o_down, o_norm, late_x, late_z,
    v_gate, v_up, v_down, v_low_gate, v_low_up, v_low_down, v_high_gate, v_high_up, v_high_down,
    v_train, v_step, l_gate, l_up, h_down,
    send_sem, line_sem, pair_sem, side_sem, extra_sem, norm_send, norm_recv, load_sem, ready,
):
    lines = shards // X
    me, w = lax.axis_index("shard"), lax.axis_index("width")
    z, x = me // X, me % X
    partner = z * X + (1 - x)
    outs = (o_gate, o_up, o_down)
    wide, tall = w_gate.shape
    unit = tall // UNITS

    head = ORDER[0][0][2] * unit
    loads = (
        (
            (low_gate, v_low_gate),
            (high_gate, v_high_gate),
            (w_gate.at[:, pl.ds(0, head)], v_gate.at[:, pl.ds(0, head)]),
        ),
        ((w_gate.at[:, pl.ds(head, tall - head)], v_gate.at[:, pl.ds(head, tall - head)]),),
        ((low_up, v_low_up), (high_up, v_high_up), (w_up, v_up)),
        ((low_down, v_low_down), (high_down, v_high_down), (w_down, v_down)),
        ((train, v_train),),
        ((step, v_step),),
    )
    for i, pairs in enumerate(loads):
        for src, dst in pairs:
            pltpu.make_async_copy(src, dst, load_sem.at[i]).start()

    def bulk(elements):
        return o_gate.at[pl.ds(0, elements // o_gate.shape[1])]

    def loaded(i):
        if len(loads[i]) == 1:
            pltpu.make_async_copy(*loads[i][0], load_sem.at[i]).wait()
        else:
            ref = bulk(sum(math.prod(dst.shape) for _, dst in loads[i]))
            pltpu.make_async_copy(ref, ref, load_sem.at[i]).wait()

    def target(way):
        return {UP: me + X, DOWN: me - X, SIDE: partner}[way]

    def has(way):
        return {UP: z + 1 < lines, DOWN: z > 0, SIDE: None}[way]

    barrier = pltpu.get_barrier_semaphore()
    peers = [lax.rem(w + k, widths) for k in range(1, widths)]
    after = [w + k < widths for k in range(1, widths)]

    def signal(sem, dev):
        pl.semaphore_signal(sem, inc=1, device_id=dev, device_id_type=MESH)

    when(has(UP), lambda: signal(barrier, (target(UP), w)))
    pl.when(x == 0)(lambda: signal(barrier, (partner, w)))
    for p, later in zip(peers, after):
        pl.when(later)(lambda p=p: signal(barrier, (me, p)))

    def enter():
        before = jnp.where(z > 0, 1, 0) + x + w
        pl.when(before > 0)(lambda: pl.semaphore_wait(barrier, before))
        when(has(DOWN), lambda: signal(ready.at[UP], (target(DOWN), w)))
        pl.when(x == 1)(lambda: signal(ready.at[SIDE], (partner, w)))
        for p, later in zip(peers, after):
            pl.when(jnp.logical_not(later))(lambda p=p: signal(ready.at[WIDE], (me, p)))

    def place(s, c):
        t, first, n = c
        block = pl.ds(pl.multiple_of(s * wide, wide), wide)
        inner = pl.ds(first * unit, n * unit)
        return outs[t].at[inner, block] if t < 2 else outs[t].at[block, inner]

    def share(t):
        return 0 if t in SHARES[0] else 1

    def receipt(way, plane, whole, extra):
        if extra:
            return extra_sem.at[0 if way == SIDE else 1]
        if way == SIDE:
            return extra_sem.at[2 + PAIR.index(whole)] if whole in PAIR else side_sem.at[share(whole[0])]
        slot = plane if way == UP else plane - 1
        for i, bundle in enumerate(BUNDLES):
            if whole in bundle:
                return line_sem.at[slot * len(BUNDLES) + i]
        return pair_sem.at[slot * 2 + (1 if whole == LATE_PAIR else 0)]

    def remote(way, s, c, whole, extra=False):
        return pltpu.make_async_remote_copy(
            src_ref=place(s, c),
            dst_ref=place(s, c),
            send_sem=send_sem.at[way * len(SHARES) + share(c[0])],
            recv_sem=receipt(way, s // X, whole, extra),
            device_id=(target(way), w),
            device_id_type=MESH,
        )

    def send(way, s, c, cond=None, whole=None, extra=False):
        when(both(cond, has(way)), lambda: remote(way, s, c, whole or c, extra).start())

    def bytes_of(units, send, recv):
        ref = bulk(units * unit * wide)
        return pltpu.make_async_remote_copy(
            src_ref=ref, dst_ref=ref, send_sem=send, recv_sem=recv, device_id=(partner, w), device_id_type=MESH
        )

    def arrive(way, plane, pieces, cond=None, extra=False):
        sem = receipt(way, plane, pieces[0], extra)
        when(cond, lambda: bytes_of(units_of(pieces), send_sem.at[0], sem).wait_recv())

    def drain(way, i, units):
        bytes_of(units, send_sem.at[way * len(SHARES) + i], side_sem.at[i]).wait_send()

    def collect(i, units):
        bytes_of(units, send_sem.at[i], side_sem.at[i]).wait_recv()

    seen = set()

    def compute(c):
        t, first, n = c
        if t not in seen:
            seen.add(t)
            loaded((0, 2, 3)[t])
            if t == 0:
                l_gate[...] = v_low_gate[...].T
            elif t == 1:
                l_up[...] = v_low_up[...].T
            else:
                h_down[...] = v_high_down[...].T
        elif c == ORDER[1][0]:
            loaded(1)
        columns = pl.ds(pl.multiple_of(me * wide, wide), wide)

        @pl.loop(0, n * unit // LANES)
        def _(i):
            at = pl.ds(pl.multiple_of(first * unit + i * LANES, LANES), LANES)
            if t < 2:
                block, low, high = ((v_gate, l_gate, v_high_gate), (v_up, l_up, v_high_up))[t]
                outs[t][at, columns] = merged(block[:, at], low[...], high[:, at]).T
            else:
                o_down[columns, at] = merged(v_down[at, :].T, h_down[...], v_low_down[:, at])

    def send_up(c, whole):
        if whole in LINE:
            send(UP, me, c, None, whole)

    enter()
    for k, (c, whole) in enumerate(ORDER):
        compute(c)
        if k == 1:
            when(has(UP), lambda: pl.semaphore_wait(ready.at[UP], 1))
            send_up(*ORDER[0])
        if whole in LINE:
            send(DOWN, me, c, None, whole)
        if k == 0:
            pl.when(x == 0)(lambda: pl.semaphore_wait(ready.at[SIDE], 1))
        else:
            send_up(c, whole)
        send(SIDE, me, c, None, whole, c == LATE_LINE)

    def norm_rows(begin, count):
        return o_norm.at[pl.ds(begin, count)]

    def norm_copy(begin, count, sem, rsem, dev):
        return pltpu.make_async_remote_copy(
            src_ref=norm_rows(begin, count), dst_ref=norm_rows(begin, count),
            send_sem=norm_send.at[sem], recv_sem=norm_recv.at[rsem],
            device_id=dev, device_id_type=MESH,
        )

    loaded(4)
    loaded(5)
    gain = v_train[...] + v_step[...]
    row = jnp.concatenate([gain] * (LANES // gain.shape[1]), axis=1)
    o_norm[pl.ds(me * widths + w, 1)] = row.reshape(1, 1, LANES)
    pl.when(w + 1 < widths)(lambda: pl.semaphore_wait(ready.at[WIDE], widths - 1 - w))
    for p in peers:
        norm_copy(me * widths + w, 1, 3, 0, (me, p)).start()
    tiles = lambda: norm_copy(0, widths - 1, 3, 0, (partner, w))
    norm_side = lambda s: norm_copy(s * widths, widths, SIDE, 1, (partner, w))
    plane_rows = X * widths
    norm_plane = lambda way, plane: norm_copy(
        plane * plane_rows, plane_rows, way, 2 + (plane if way == UP else plane - 1), (target(way), w)
    )
    if widths > 1:
        tiles().wait_recv()
    norm_side(me).start()

    far = far_plane(z, lines)
    inner = jnp.logical_and(z > 0, z + 1 < lines)
    lower = z < lines // 2
    mate = jnp.where(lower, z + 1, z - 1)
    lends = {
        DOWN: jnp.logical_and(z >= 2, z - 1 < lines // 2),
        UP: jnp.logical_and(z + 1 >= lines // 2, z + 2 < lines),
    }

    def by_side(plane):
        return jnp.logical_and(plane != far, jnp.logical_not(jnp.logical_and(inner, plane == mate)))

    def lend():
        arrive(SIDE, z, (LATE_LINE,), None, True)
        for way in (UP, DOWN):
            send(way, partner, LATE_LINE, lends[way], None, True)

    def hops(d):
        return ((UP, z - d, z >= d), (DOWN, z + d, z + d < lines))

    def forward_line(d):
        for pieces in BUNDLES:
            for way, plane, cond in hops(d):
                arrive(way, plane, pieces, cond)
                for c in pieces:
                    send(way, plane * X + x, c, cond)
                    send(SIDE, plane * X + x, c, both(cond, by_side(plane)) if c == LATE_LINE else cond)

    source = {UP: 0, DOWN: lines - 1}
    feeds = {UP: z == lines - 2, DOWN: z == 1}

    def send_pair(way, plane, j, c, cond=None):
        if c == LATE_PAIR:
            late = jnp.logical_and(feeds[way], plane == source[way])
            cond = both(cond, jnp.logical_not(late))
        send(way, plane * X + (x + j) % X, c, cond)

    def arrive_pair(way, plane, pieces, cond):
        if LATE_PAIR in pieces:
            end = {UP: z == lines - 1, DOWN: z == 0}[way]
            late = jnp.logical_and(end, plane == source[way])
            cond = both(cond, jnp.logical_not(late))
        arrive(way, plane, pieces, cond)

    def forward_pair(d):
        if d == 0:
            send(UP, me, WHOLE)
            send(DOWN, me, WHOLE)
            norm_side(partner).wait_recv()
            for way in (UP, DOWN):
                when(has(way), lambda way=way: norm_plane(way, z).start())
            for c in PAIR:
                arrive(SIDE, z, (c,))
                send_pair(UP, z, 1, c)
                send_pair(DOWN, z, 1, c)
            return
        for way, plane, cond in hops(d):
            when(cond, lambda way=way, plane=plane: norm_plane(way, plane).wait_recv())
            when(both(cond, has(way)), lambda way=way, plane=plane: norm_plane(way, plane).start())
        for bundle in (((WHOLE, 0), (PAIR[0], 1)), ((LATE_PAIR, 1),)):
            for way, plane, cond in hops(d):
                arrive_pair(way, plane, [c for c, _ in bundle], cond)
                for c, j in bundle:
                    send_pair(way, plane, j, c, cond)

    for d in range(1, lines):
        forward_line(d)
        forward_pair(d - 1)
        if d == 1:
            lend()
    bridge = jnp.logical_or(z == 1, z == lines - 2)
    keep = jnp.where(z == 1, lines - 1, 0) * X + (1 - x)
    keep = jnp.where(bridge, keep, me)
    late_x[...] = place(far * X + x, LATE_LINE)[...]
    late_z[...] = place(keep, LATE_PAIR)[...]
    forward_pair(lines - 1)

    arrive(DOWN, mate, (LATE_LINE,), inner, True)
    lent = share(LATE_LINE[0])
    for i, arrays in enumerate(SHARES):
        units = lines * units_of(LINE, arrays)
        own = units_of(PAIR, arrays)
        if i != lent:
            collect(i, units)
            drain(SIDE, i, units + own)
            continue
        for cond, skipped in ((inner, 2 * LATE_LINE[2]), (jnp.logical_not(inner), LATE_LINE[2])):

            @pl.when(cond)
            def _(i=i, units=units - skipped, own=own):
                collect(i, units - LATE_LINE[2])
                drain(SIDE, i, units + own)
    norm_side(me).wait_send()
    if widths > 1:
        tiles().wait_send()
    for way in (UP, DOWN):
        for k in range(lines):
            planes = k + 1 if way == UP else lines - k
            if planes == lines:
                continue

            @pl.when(both(z == k, has(way)))
            def _(way=way, planes=planes):
                feeder = k == (lines - 2 if way == UP else 1)
                lends_here = (k >= 2 and k - 1 < lines // 2) if way == DOWN else (k + 1 >= lines // 2 and k + 2 < lines)
                for i, arrays in enumerate(SHARES):
                    units = planes * (units_of(LINE, arrays) + X * units_of(PAIR, arrays))
                    units -= LATE_PAIR[2] * (feeder and i == share(LATE_PAIR[0]))
                    units += LATE_LINE[2] * (lends_here and i == lent)
                    drain(way, i, units)
                norm_copy(0, planes * plane_rows, way, 0, (partner, w)).wait_send()


def gather_all(shards, widths, args):
    lines = shards // X
    w_gate, low_gate, high_gate, w_up, low_up, high_up, w_down, low_down, high_down, train, step = args
    hbm = pl.BlockSpec(memory_space=pltpu.HBM)
    vmem = pl.BlockSpec(memory_space=pltpu.VMEM)
    like = lambda a: pltpu.VMEM(a.shape, a.dtype)
    flip = lambda a: pltpu.VMEM(a.shape[::-1], a.dtype)
    wide, tall = w_gate.shape
    full = pltpu.VMEM((tall, shards * wide), w_gate.dtype)
    return pl.pallas_call(
        functools.partial(gather_kernel, shards, widths),
        out_shape=(
            full, full,
            pltpu.VMEM((shards * wide, tall), w_down.dtype),
            pltpu.VMEM((shards * widths, 1, LANES), train.dtype),
            pltpu.VMEM((wide, LATE_LINE[2] * tall // UNITS), w_down.dtype),
            pltpu.VMEM((LATE_PAIR[2] * tall // UNITS, wide), w_up.dtype),
        ),
        in_specs=[hbm] * len(args),
        out_specs=(vmem,) * 6,
        scratch_shapes=[
            like(w_gate), like(w_up), like(w_down),
            like(low_gate), like(low_up), like(low_down),
            like(high_gate), like(high_up), like(high_down),
            like(train), like(step),
            flip(low_gate), flip(low_up), flip(high_down),
            pltpu.SemaphoreType.DMA((WAYS * len(SHARES),)),
            pltpu.SemaphoreType.DMA(((lines - 1) * len(BUNDLES),)),
            pltpu.SemaphoreType.DMA(((lines - 1) * 2,)),
            pltpu.SemaphoreType.DMA((len(SHARES),)),
            pltpu.SemaphoreType.DMA((2 + len(PAIR),)),
            pltpu.SemaphoreType.DMA((4,)),
            pltpu.SemaphoreType.DMA((1 + lines,)),
            pltpu.SemaphoreType.DMA((6,)),
            pltpu.SemaphoreType.REGULAR((3,)),
        ],
        compiler_params=pltpu.CompilerParams(collective_id=0, has_side_effects=True, vmem_limit_bytes=16 * 2**20),
    )(*(pltpu.with_memory_space_constraint(a, pltpu.HBM) for a in args))


def write_kernel(gate, up, down, rows, o_gate, o_up, o_down, o_norm, norm, sem):
    pairs = ((gate, o_gate), (up, o_up), (down, o_down))
    part = gate.shape[0] // WRITES
    copies = [
        pltpu.make_async_copy(a.at[pl.ds(j * part, part)], b.at[pl.ds(j * part, part)], sem.at[i])
        for i, (a, b) in enumerate(pairs)
        for j in range(WRITES)
    ]
    for copy in copies:
        copy.start()
    per = rows.shape[1]
    lane = lax.broadcasted_iota(jnp.int32, norm.shape, 1) // (LANES // per)
    line = rows[:, 0, :]
    for j in range(1, per):
        line = jnp.where(lane == j, rows[:, j, :], line)
    norm[...] = line.astype(norm.dtype)
    last = pltpu.make_async_copy(norm, o_norm, sem.at[len(pairs)])
    last.start()
    for i, (a, b) in enumerate(pairs):
        pltpu.make_async_copy(a, b, sem.at[i]).wait()
    last.wait()


def write_out(gate, up, down, rows):
    any_ = pl.BlockSpec(memory_space=pl.ANY)
    vmem = pl.BlockSpec(memory_space=pltpu.VMEM)
    norm = (rows.shape[0], LANES)
    return pl.pallas_call(
        write_kernel,
        out_shape=tuple(jax.ShapeDtypeStruct(a.shape, a.dtype) for a in (gate, up, down))
        + (jax.ShapeDtypeStruct(norm, jnp.bfloat16),),
        in_specs=[any_] * 3 + [vmem],
        out_specs=(any_,) * 4,
        scratch_shapes=[pltpu.VMEM(norm, jnp.bfloat16), pltpu.SemaphoreType.DMA((4,))],
        cost_estimate=pl.CostEstimate(flops=WRITE_FLOPS, bytes_accessed=2 * 3 * gate.size * 2, transcendentals=0),
        compiler_params=pltpu.CompilerParams(vmem_limit_bytes=4 * 2**20),
    )(gate, up, down, rows)


def late_kernel(lines, up, down, late_z, late_x, o_up, o_down, sem):
    me = lax.axis_index("shard")
    z, x = me // X, me % X
    wide, tall = late_z.shape[1], up.shape[0]
    unit = tall // UNITS
    end = jnp.logical_or(z == 0, z == lines - 1)
    block = (far_plane(z, lines) * X + (1 - x)) * wide
    block = pl.ds(pl.multiple_of(block, wide), wide)
    inner = lambda c: pl.ds(c[1] * unit, c[2] * unit)
    put_x = pltpu.make_async_copy(late_x, o_down.at[block, inner(LATE_LINE)], sem.at[0])
    put_z = pltpu.make_async_copy(late_z, o_up.at[inner(LATE_PAIR), block], sem.at[1])
    put_x.start()
    pl.when(end)(put_z.start)
    put_x.wait()
    pl.when(end)(put_z.wait)


def write_late(lines, up, down, late_x, late_z):
    any_ = pl.BlockSpec(memory_space=pl.ANY)
    vmem = pl.BlockSpec(memory_space=pltpu.VMEM)
    return pl.pallas_call(
        functools.partial(late_kernel, lines),
        out_shape=tuple(jax.ShapeDtypeStruct(a.shape, a.dtype) for a in (up, down)),
        in_specs=[any_] * 2 + [vmem] * 2,
        out_specs=(any_,) * 2,
        input_output_aliases={0: 0, 1: 1},
        scratch_shapes=[pltpu.SemaphoreType.DMA((2,))],
        compiler_params=pltpu.CompilerParams(vmem_limit_bytes=4 * 2**20),
    )(up, down, late_z, late_x)


def body(
    shards,
    widths,
    w_gate,
    low_gate,
    high_gate,
    w_up,
    low_up,
    high_up,
    w_down,
    low_down,
    high_down,
    norm_train,
    norm_step,
):
    count = norm_train.shape[0]
    wide, tall = w_gate.shape
    if shards % (2 * X) or shards > 4 * X or wide % LANES or tall % (UNITS * LANES) or LANES % count or (shards * widths * count) % LANES:
        gate = merged(w_gate, low_gate, high_gate)
        up = merged(w_up, low_up, high_up)
        down = merged(w_down, low_down, high_down)
        gate, up, down = (
            lax.all_gather(gate, "shard", axis=0, tiled=True),
            lax.all_gather(up, "shard", axis=0, tiled=True),
            lax.all_gather(down, "shard", axis=1, tiled=True),
        )
        gain = (norm_train + norm_step).astype(jnp.bfloat16)
        gain = lax.all_gather(gain, ("shard", "width"), axis=0, tiled=True)
        return gate.T, up.T, down.T, gain
    args = (
        w_gate, low_gate.T, high_gate, w_up, low_up.T, high_up, w_down, low_down.T, high_down,
        norm_train.reshape(1, count), norm_step.reshape(1, count),
    )
    gate, up, down, rows, late_x, late_z = gather_all(shards, widths, args)
    per = LANES // count
    late_z = lax.ppermute(late_z, "shard", [(s, s ^ X) for s in range(shards)])
    late_x = lax.ppermute(late_x, "shard", [(s, s ^ 1) for s in range(shards)])
    gate, up, down, norm = write_out(gate, up, down, rows.reshape(-1, per, LANES))
    up, down = write_late(shards // X, up, down, late_x, late_z)
    return gate, up, down, norm.reshape(-1)


def solution(mesh):
    return jax.shard_map(
        functools.partial(body, mesh.shape["shard"], mesh.shape["width"]),
        mesh=mesh,
        in_specs=(
            P("shard", "width"),
            P("shard", None),
            P(None, "width"),
            P("shard", "width"),
            P("shard", None),
            P(None, "width"),
            P("width", "shard"),
            P("width", None),
            P(None, "shard"),
            P(("shard", "width")),
            P(("shard", "width")),
        ),
        out_specs=(P("width", None), P("width", None), P(None, "width"), P()),
        check_vma=False,
    )
```

```python
import functools
import math

import jax
import jax.numpy as jnp
from jax import lax
from jax.experimental import pallas as pl
from jax.experimental.pallas import tpu as pltpu
from jax.sharding import PartitionSpec as P

mix_rate = 2.0
MESH = pl.DeviceIdType.MESH
X = 2
LANES = 128

UNITS = 16
LINE = ((0, 0, 16), (1, 0, 8), (2, 0, 10), (2, 10, 6))
PAIR = ((1, 8, 2), (1, 10, 6))
WHOLE = (1, 8, 8)
BUNDLES = (LINE[:1], LINE[1:3], LINE[3:])
LATE_LINE, LATE_PAIR = LINE[-1], PAIR[-1]
ORDER = (
    ((0, 0, 1), LINE[0]), ((0, 1, 3), LINE[0]), ((0, 4, 12), LINE[0]),
    (PAIR[0], PAIR[0]), (PAIR[1], PAIR[1]),
    (LINE[1], LINE[1]), (LINE[2], LINE[2]), (LINE[3], LINE[3]),
)
UP, DOWN, SIDE = 0, 1, 2
WIDE = DOWN
WAYS = 3
WRITES = 4
WRITE_FLOPS = 2 * 10**9


def units_of(pieces, arrays=(0, 1, 2)):
    return sum(n for array, _, n in pieces if array in arrays)


SHARES = ((0, 1), (2,))


def merged(w, low, high):
    fresh = w.astype(jnp.float32) + mix_rate * jnp.dot(
        low, high, preferred_element_type=jnp.float32
    )
    return fresh.astype(jnp.bfloat16)


def when(cond, fn):
    if cond is None:
        fn()
    else:
        pl.when(cond)(fn)


def both(a, b):
    if a is None:
        return b
    if b is None:
        return a
    return jnp.logical_and(a, b)


def far_plane(z, lines):
    return jnp.where(z < lines // 2, lines - 1, 0)


def gather_kernel(
    shards, widths,
    w_gate, low_gate, high_gate, w_up, low_up, high_up, w_down, low_down, high_down, train, step,
    o_gate, o_up, o_down, o_norm, late_x, late_z,
    v_gate, v_up, v_down, v_low_gate, v_low_up, v_low_down, v_high_gate, v_high_up, v_high_down,
    v_train, v_step, l_gate, l_up, h_down,
    send_sem, line_sem, pair_sem, side_sem, extra_sem, norm_send, norm_recv, load_sem, ready,
):
    lines = shards // X
    me, w = lax.axis_index("shard"), lax.axis_index("width")
    z, x = me // X, me % X
    partner = z * X + (1 - x)
    outs = (o_gate, o_up, o_down)
    wide, tall = w_gate.shape
    unit = tall // UNITS

    head = ORDER[0][0][2] * unit
    loads = (
        (
            (low_gate, v_low_gate),
            (high_gate, v_high_gate),
            (w_gate.at[:, pl.ds(0, head)], v_gate.at[:, pl.ds(0, head)]),
        ),
        ((w_gate.at[:, pl.ds(head, tall - head)], v_gate.at[:, pl.ds(head, tall - head)]),),
        ((low_up, v_low_up), (high_up, v_high_up), (w_up, v_up)),
        ((low_down, v_low_down), (high_down, v_high_down), (w_down, v_down)),
        ((train, v_train),),
        ((step, v_step),),
    )
    for i, pairs in enumerate(loads):
        for src, dst in pairs:
            pltpu.make_async_copy(src, dst, load_sem.at[i]).start()

    def bulk(elements):
        return o_gate.at[pl.ds(0, elements // o_gate.shape[1])]

    def loaded(i):
        if len(loads[i]) == 1:
            pltpu.make_async_copy(*loads[i][0], load_sem.at[i]).wait()
        else:
            ref = bulk(sum(math.prod(dst.shape) for _, dst in loads[i]))
            pltpu.make_async_copy(ref, ref, load_sem.at[i]).wait()

    def target(way):
        return {UP: me + X, DOWN: me - X, SIDE: partner}[way]

    def has(way):
        return {UP: z + 1 < lines, DOWN: z > 0, SIDE: None}[way]

    barrier = pltpu.get_barrier_semaphore()
    peers = [lax.rem(w + k, widths) for k in range(1, widths)]
    after = [w + k < widths for k in range(1, widths)]

    def signal(sem, dev):
        pl.semaphore_signal(sem, inc=1, device_id=dev, device_id_type=MESH)

    when(has(UP), lambda: signal(barrier, (target(UP), w)))
    pl.when(x == 0)(lambda: signal(barrier, (partner, w)))
    for p, later in zip(peers, after):
        pl.when(later)(lambda p=p: signal(barrier, (me, p)))

    def enter():
        before = jnp.where(z > 0, 1, 0) + x + w
        pl.when(before > 0)(lambda: pl.semaphore_wait(barrier, before))
        when(has(DOWN), lambda: signal(ready.at[UP], (target(DOWN), w)))
        pl.when(x == 1)(lambda: signal(ready.at[SIDE], (partner, w)))
        for p, later in zip(peers, after):
            pl.when(jnp.logical_not(later))(lambda p=p: signal(ready.at[WIDE], (me, p)))

    def place(s, c):
        t, first, n = c
        block = pl.ds(pl.multiple_of(s * wide, wide), wide)
        inner = pl.ds(first * unit, n * unit)
        return outs[t].at[inner, block] if t < 2 else outs[t].at[block, inner]

    def share(t):
        return 0 if t in SHARES[0] else 1

    def receipt(way, plane, whole, extra):
        if extra:
            return extra_sem.at[0 if way == SIDE else 1]
        if way == SIDE:
            return extra_sem.at[2 + PAIR.index(whole)] if whole in PAIR else side_sem.at[share(whole[0])]
        slot = plane if way == UP else plane - 1
        for i, bundle in enumerate(BUNDLES):
            if whole in bundle:
                return line_sem.at[slot * len(BUNDLES) + i]
        return pair_sem.at[slot * 2 + (1 if whole == LATE_PAIR else 0)]

    def remote(way, s, c, whole, extra=False):
        return pltpu.make_async_remote_copy(
            src_ref=place(s, c),
            dst_ref=place(s, c),
            send_sem=send_sem.at[way * len(SHARES) + share(c[0])],
            recv_sem=receipt(way, s // X, whole, extra),
            device_id=(target(way), w),
            device_id_type=MESH,
        )

    def send(way, s, c, cond=None, whole=None, extra=False):
        when(both(cond, has(way)), lambda: remote(way, s, c, whole or c, extra).start())

    def bytes_of(units, send, recv):
        ref = bulk(units * unit * wide)
        return pltpu.make_async_remote_copy(
            src_ref=ref, dst_ref=ref, send_sem=send, recv_sem=recv, device_id=(partner, w), device_id_type=MESH
        )

    def arrive(way, plane, pieces, cond=None, extra=False):
        sem = receipt(way, plane, pieces[0], extra)
        when(cond, lambda: bytes_of(units_of(pieces), send_sem.at[0], sem).wait_recv())

    def drain(way, i, units):
        bytes_of(units, send_sem.at[way * len(SHARES) + i], side_sem.at[i]).wait_send()

    def collect(i, units):
        bytes_of(units, send_sem.at[i], side_sem.at[i]).wait_recv()

    seen = set()

    def compute(c):
        t, first, n = c
        if t not in seen:
            seen.add(t)
            loaded((0, 2, 3)[t])
            if t == 0:
                l_gate[...] = v_low_gate[...].T
            elif t == 1:
                l_up[...] = v_low_up[...].T
            else:
                h_down[...] = v_high_down[...].T
        elif c == ORDER[1][0]:
            loaded(1)
        columns = pl.ds(pl.multiple_of(me * wide, wide), wide)

        @pl.loop(0, n * unit // LANES)
        def _(i):
            at = pl.ds(pl.multiple_of(first * unit + i * LANES, LANES), LANES)
            if t < 2:
                block, low, high = ((v_gate, l_gate, v_high_gate), (v_up, l_up, v_high_up))[t]
                outs[t][at, columns] = merged(block[:, at], low[...], high[:, at]).T
            else:
                o_down[columns, at] = merged(v_down[at, :].T, h_down[...], v_low_down[:, at])

    def send_up(c, whole):
        if whole in LINE:
            send(UP, me, c, None, whole)

    for k, (c, whole) in enumerate(ORDER):
        compute(c)
        if k == 0:
            enter()
        if k == 1:
            when(has(UP), lambda: pl.semaphore_wait(ready.at[UP], 1))
            send_up(*ORDER[0])
        if whole in LINE:
            send(DOWN, me, c, None, whole)
        if k == 0:
            pl.when(x == 0)(lambda: pl.semaphore_wait(ready.at[SIDE], 1))
        else:
            send_up(c, whole)
        send(SIDE, me, c, None, whole, c == LATE_LINE)

    def norm_rows(begin, count):
        return o_norm.at[pl.ds(begin, count)]

    def norm_copy(begin, count, sem, rsem, dev):
        return pltpu.make_async_remote_copy(
            src_ref=norm_rows(begin, count), dst_ref=norm_rows(begin, count),
            send_sem=norm_send.at[sem], recv_sem=norm_recv.at[rsem],
            device_id=dev, device_id_type=MESH,
        )

    loaded(4)
    loaded(5)
    gain = v_train[...] + v_step[...]
    row = jnp.concatenate([gain] * (LANES // gain.shape[1]), axis=1)
    o_norm[pl.ds(me * widths + w, 1)] = row.reshape(1, 1, LANES)
    pl.when(w + 1 < widths)(lambda: pl.semaphore_wait(ready.at[WIDE], widths - 1 - w))
    for p in peers:
        norm_copy(me * widths + w, 1, 3, 0, (me, p)).start()
    tiles = lambda: norm_copy(0, widths - 1, 3, 0, (partner, w))
    norm_side = lambda s: norm_copy(s * widths, widths, SIDE, 1, (partner, w))
    plane_rows = X * widths
    norm_plane = lambda way, plane: norm_copy(
        plane * plane_rows, plane_rows, way, 2 + (plane if way == UP else plane - 1), (target(way), w)
    )
    if widths > 1:
        tiles().wait_recv()
    norm_side(me).start()

    far = far_plane(z, lines)
    inner = jnp.logical_and(z > 0, z + 1 < lines)
    lower = z < lines // 2
    mate = jnp.where(lower, z + 1, z - 1)
    lends = {
        DOWN: jnp.logical_and(z >= 2, z - 1 < lines // 2),
        UP: jnp.logical_and(z + 1 >= lines // 2, z + 2 < lines),
    }

    def by_side(plane):
        return jnp.logical_and(plane != far, jnp.logical_not(jnp.logical_and(inner, plane == mate)))

    def lend():
        arrive(SIDE, z, (LATE_LINE,), None, True)
        for way in (UP, DOWN):
            send(way, partner, LATE_LINE, lends[way], None, True)

    def hops(d):
        return ((UP, z - d, z >= d), (DOWN, z + d, z + d < lines))

    def forward_line(d):
        for pieces in BUNDLES:
            for way, plane, cond in hops(d):
                arrive(way, plane, pieces, cond)
                for c in pieces:
                    send(way, plane * X + x, c, cond)
                    send(SIDE, plane * X + x, c, both(cond, by_side(plane)) if c == LATE_LINE else cond)

    source = {UP: 0, DOWN: lines - 1}
    feeds = {UP: z == lines - 2, DOWN: z == 1}

    def send_pair(way, plane, j, c, cond=None):
        if c == LATE_PAIR:
            late = jnp.logical_and(feeds[way], plane == source[way])
            cond = both(cond, jnp.logical_not(late))
        send(way, plane * X + (x + j) % X, c, cond)

    def arrive_pair(way, plane, pieces, cond):
        if LATE_PAIR in pieces:
            end = {UP: z == lines - 1, DOWN: z == 0}[way]
            late = jnp.logical_and(end, plane == source[way])
            cond = both(cond, jnp.logical_not(late))
        arrive(way, plane, pieces, cond)

    def forward_pair(d):
        if d == 0:
            send(UP, me, WHOLE)
            send(DOWN, me, WHOLE)
            norm_side(partner).wait_recv()
            for way in (UP, DOWN):
                when(has(way), lambda way=way: norm_plane(way, z).start())
            for c in PAIR:
                arrive(SIDE, z, (c,))
                send_pair(UP, z, 1, c)
                send_pair(DOWN, z, 1, c)
            return
        for way, plane, cond in hops(d):
            when(cond, lambda way=way, plane=plane: norm_plane(way, plane).wait_recv())
            when(both(cond, has(way)), lambda way=way, plane=plane: norm_plane(way, plane).start())
        for bundle in (((WHOLE, 0), (PAIR[0], 1)), ((LATE_PAIR, 1),)):
            for way, plane, cond in hops(d):
                arrive_pair(way, plane, [c for c, _ in bundle], cond)
                for c, j in bundle:
                    send_pair(way, plane, j, c, cond)

    for d in range(1, lines):
        forward_line(d)
        forward_pair(d - 1)
        if d == 1:
            lend()
    bridge = jnp.logical_or(z == 1, z == lines - 2)
    keep = jnp.where(z == 1, lines - 1, 0) * X + (1 - x)
    keep = jnp.where(bridge, keep, me)
    late_x[...] = place(far * X + x, LATE_LINE)[...]
    late_z[...] = place(keep, LATE_PAIR)[...]
    forward_pair(lines - 1)

    arrive(DOWN, mate, (LATE_LINE,), inner, True)
    lent = share(LATE_LINE[0])
    for i, arrays in enumerate(SHARES):
        units = lines * units_of(LINE, arrays)
        own = units_of(PAIR, arrays)
        if i != lent:
            collect(i, units)
            drain(SIDE, i, units + own)
            continue
        for cond, skipped in ((inner, 2 * LATE_LINE[2]), (jnp.logical_not(inner), LATE_LINE[2])):

            @pl.when(cond)
            def _(i=i, units=units - skipped, own=own):
                collect(i, units - LATE_LINE[2])
                drain(SIDE, i, units + own)
    norm_side(me).wait_send()
    if widths > 1:
        tiles().wait_send()
    for way in (UP, DOWN):
        for k in range(lines):
            planes = k + 1 if way == UP else lines - k
            if planes == lines:
                continue

            @pl.when(both(z == k, has(way)))
            def _(way=way, planes=planes):
                feeder = k == (lines - 2 if way == UP else 1)
                lends_here = (k >= 2 and k - 1 < lines // 2) if way == DOWN else (k + 1 >= lines // 2 and k + 2 < lines)
                for i, arrays in enumerate(SHARES):
                    units = planes * (units_of(LINE, arrays) + X * units_of(PAIR, arrays))
                    units -= LATE_PAIR[2] * (feeder and i == share(LATE_PAIR[0]))
                    units += LATE_LINE[2] * (lends_here and i == lent)
                    drain(way, i, units)
                norm_copy(0, planes * plane_rows, way, 0, (partner, w)).wait_send()


def gather_all(shards, widths, args):
    lines = shards // X
    w_gate, low_gate, high_gate, w_up, low_up, high_up, w_down, low_down, high_down, train, step = args
    hbm = pl.BlockSpec(memory_space=pltpu.HBM)
    vmem = pl.BlockSpec(memory_space=pltpu.VMEM)
    like = lambda a: pltpu.VMEM(a.shape, a.dtype)
    flip = lambda a: pltpu.VMEM(a.shape[::-1], a.dtype)
    wide, tall = w_gate.shape
    full = pltpu.VMEM((tall, shards * wide), w_gate.dtype)
    return pl.pallas_call(
        functools.partial(gather_kernel, shards, widths),
        out_shape=(
            full, full,
            pltpu.VMEM((shards * wide, tall), w_down.dtype),
            pltpu.VMEM((shards * widths, 1, LANES), train.dtype),
            pltpu.VMEM((wide, LATE_LINE[2] * tall // UNITS), w_down.dtype),
            pltpu.VMEM((LATE_PAIR[2] * tall // UNITS, wide), w_up.dtype),
        ),
        in_specs=[hbm] * len(args),
        out_specs=(vmem,) * 6,
        scratch_shapes=[
            like(w_gate), like(w_up), like(w_down),
            like(low_gate), like(low_up), like(low_down),
            like(high_gate), like(high_up), like(high_down),
            like(train), like(step),
            flip(low_gate), flip(low_up), flip(high_down),
            pltpu.SemaphoreType.DMA((WAYS * len(SHARES),)),
            pltpu.SemaphoreType.DMA(((lines - 1) * len(BUNDLES),)),
            pltpu.SemaphoreType.DMA(((lines - 1) * 2,)),
            pltpu.SemaphoreType.DMA((len(SHARES),)),
            pltpu.SemaphoreType.DMA((2 + len(PAIR),)),
            pltpu.SemaphoreType.DMA((4,)),
            pltpu.SemaphoreType.DMA((1 + lines,)),
            pltpu.SemaphoreType.DMA((6,)),
            pltpu.SemaphoreType.REGULAR((3,)),
        ],
        compiler_params=pltpu.CompilerParams(collective_id=0, has_side_effects=True, vmem_limit_bytes=16 * 2**20),
    )(*(pltpu.with_memory_space_constraint(a, pltpu.HBM) for a in args))


def write_kernel(gate, up, down, rows, o_gate, o_up, o_down, o_norm, norm, sem):
    pairs = ((gate, o_gate), (up, o_up), (down, o_down))
    part = gate.shape[0] // WRITES
    copies = [
        pltpu.make_async_copy(a.at[pl.ds(j * part, part)], b.at[pl.ds(j * part, part)], sem.at[i])
        for i, (a, b) in enumerate(pairs)
        for j in range(WRITES)
    ]
    for copy in copies:
        copy.start()
    per = rows.shape[1]
    lane = lax.broadcasted_iota(jnp.int32, norm.shape, 1) // (LANES // per)
    line = rows[:, 0, :]
    for j in range(1, per):
        line = jnp.where(lane == j, rows[:, j, :], line)
    norm[...] = line.astype(norm.dtype)
    last = pltpu.make_async_copy(norm, o_norm, sem.at[len(pairs)])
    last.start()
    for i, (a, b) in enumerate(pairs):
        pltpu.make_async_copy(a, b, sem.at[i]).wait()
    last.wait()


def write_out(gate, up, down, rows):
    any_ = pl.BlockSpec(memory_space=pl.ANY)
    vmem = pl.BlockSpec(memory_space=pltpu.VMEM)
    norm = (rows.shape[0], LANES)
    return pl.pallas_call(
        write_kernel,
        out_shape=tuple(jax.ShapeDtypeStruct(a.shape, a.dtype) for a in (gate, up, down))
        + (jax.ShapeDtypeStruct(norm, jnp.bfloat16),),
        in_specs=[any_] * 3 + [vmem],
        out_specs=(any_,) * 4,
        scratch_shapes=[pltpu.VMEM(norm, jnp.bfloat16), pltpu.SemaphoreType.DMA((4,))],
        cost_estimate=pl.CostEstimate(flops=WRITE_FLOPS, bytes_accessed=2 * 3 * gate.size * 2, transcendentals=0),
        compiler_params=pltpu.CompilerParams(vmem_limit_bytes=4 * 2**20),
    )(gate, up, down, rows)


def late_kernel(lines, up, down, late_z, late_x, o_up, o_down, sem):
    me = lax.axis_index("shard")
    z, x = me // X, me % X
    wide, tall = late_z.shape[1], up.shape[0]
    unit = tall // UNITS
    end = jnp.logical_or(z == 0, z == lines - 1)
    block = (far_plane(z, lines) * X + (1 - x)) * wide
    block = pl.ds(pl.multiple_of(block, wide), wide)
    inner = lambda c: pl.ds(c[1] * unit, c[2] * unit)
    put_x = pltpu.make_async_copy(late_x, o_down.at[block, inner(LATE_LINE)], sem.at[0])
    put_z = pltpu.make_async_copy(late_z, o_up.at[inner(LATE_PAIR), block], sem.at[1])
    put_x.start()
    pl.when(end)(put_z.start)
    put_x.wait()
    pl.when(end)(put_z.wait)


def write_late(lines, up, down, late_x, late_z):
    any_ = pl.BlockSpec(memory_space=pl.ANY)
    vmem = pl.BlockSpec(memory_space=pltpu.VMEM)
    return pl.pallas_call(
        functools.partial(late_kernel, lines),
        out_shape=tuple(jax.ShapeDtypeStruct(a.shape, a.dtype) for a in (up, down)),
        in_specs=[any_] * 2 + [vmem] * 2,
        out_specs=(any_,) * 2,
        input_output_aliases={0: 0, 1: 1},
        scratch_shapes=[pltpu.SemaphoreType.DMA((2,))],
        compiler_params=pltpu.CompilerParams(vmem_limit_bytes=4 * 2**20),
    )(up, down, late_z, late_x)


def body(
    shards,
    widths,
    w_gate,
    low_gate,
    high_gate,
    w_up,
    low_up,
    high_up,
    w_down,
    low_down,
    high_down,
    norm_train,
    norm_step,
):
    count = norm_train.shape[0]
    wide, tall = w_gate.shape
    if shards % (2 * X) or shards > 4 * X or wide % LANES or tall % (UNITS * LANES) or LANES % count or (shards * widths * count) % LANES:
        gate = merged(w_gate, low_gate, high_gate)
        up = merged(w_up, low_up, high_up)
        down = merged(w_down, low_down, high_down)
        gate, up, down = (
            lax.all_gather(gate, "shard", axis=0, tiled=True),
            lax.all_gather(up, "shard", axis=0, tiled=True),
            lax.all_gather(down, "shard", axis=1, tiled=True),
        )
        gain = (norm_train + norm_step).astype(jnp.bfloat16)
        gain = lax.all_gather(gain, ("shard", "width"), axis=0, tiled=True)
        return gate.T, up.T, down.T, gain
    args = (
        w_gate, low_gate.T, high_gate, w_up, low_up.T, high_up, w_down, low_down.T, high_down,
        norm_train.reshape(1, count), norm_step.reshape(1, count),
    )
    gate, up, down, rows, late_x, late_z = gather_all(shards, widths, args)
    per = LANES // count
    late_z = lax.ppermute(late_z, "shard", [(s, s ^ X) for s in range(shards)])
    late_x = lax.ppermute(late_x, "shard", [(s, s ^ 1) for s in range(shards)])
    gate, up, down, norm = write_out(gate, up, down, rows.reshape(-1, per, LANES))
    up, down = write_late(shards // X, up, down, late_x, late_z)
    return gate, up, down, norm.reshape(-1)


def solution(mesh):
    return jax.shard_map(
        functools.partial(body, mesh.shape["shard"], mesh.shape["width"]),
        mesh=mesh,
        in_specs=(
            P("shard", "width"),
            P("shard", None),
            P(None, "width"),
            P("shard", "width"),
            P("shard", None),
            P(None, "width"),
            P("width", "shard"),
            P("width", None),
            P(None, "shard"),
            P(("shard", "width")),
            P(("shard", "width")),
        ),
        out_specs=(P("width", None), P("width", None), P(None, "width"), P()),
        check_vma=False,
    )
```

```python
import functools
import math

import jax
import jax.numpy as jnp
from jax import lax
from jax.experimental import pallas as pl
from jax.experimental.pallas import tpu as pltpu
from jax.sharding import PartitionSpec as P

mix_rate = 2.0
MESH = pl.DeviceIdType.MESH
X = 2
LANES = 128

UNITS = 16
LINE = ((0, 0, 16), (1, 0, 8), (2, 0, 10), (2, 10, 6))
PAIR = ((1, 8, 2), (1, 10, 6))
WHOLE = (1, 8, 8)
BUNDLES = (LINE[:1], LINE[1:3], LINE[3:])
LATE_LINE, LATE_PAIR = LINE[-1], PAIR[-1]
ORDER = (
    ((0, 0, 1), LINE[0]), ((0, 1, 3), LINE[0]), ((0, 4, 12), LINE[0]),
    (PAIR[0], PAIR[0]), (PAIR[1], PAIR[1]),
    (LINE[1], LINE[1]), (LINE[2], LINE[2]), (LINE[3], LINE[3]),
)
UP, DOWN, SIDE = 0, 1, 2
WIDE = DOWN
WAYS = 3
WRITES = 4
WRITE_FLOPS = 2 * 10**9


def units_of(pieces, arrays=(0, 1, 2)):
    return sum(n for array, _, n in pieces if array in arrays)


SHARES = ((0, 1), (2,))


def merged(w, low, high):
    fresh = w.astype(jnp.float32) + mix_rate * jnp.dot(
        low, high, preferred_element_type=jnp.float32
    )
    return fresh.astype(jnp.bfloat16)


def when(cond, fn):
    if cond is None:
        fn()
    else:
        pl.when(cond)(fn)


def both(a, b):
    if a is None:
        return b
    if b is None:
        return a
    return jnp.logical_and(a, b)


def far_plane(z, lines):
    return jnp.where(z < lines // 2, lines - 1, 0)


def gather_kernel(
    shards, widths,
    w_gate, low_gate, high_gate, w_up, low_up, high_up, w_down, low_down, high_down, train, step,
    o_gate, o_up, o_down, o_norm, late_x, late_z,
    v_gate, v_up, v_down, v_low_gate, v_low_up, v_low_down, v_high_gate, v_high_up, v_high_down,
    v_train, v_step, l_gate, l_up, h_down,
    send_sem, line_sem, pair_sem, side_sem, extra_sem, norm_send, norm_recv, load_sem, ready,
):
    lines = shards // X
    me, w = lax.axis_index("shard"), lax.axis_index("width")
    z, x = me // X, me % X
    partner = z * X + (1 - x)
    outs = (o_gate, o_up, o_down)
    wide, tall = w_gate.shape
    unit = tall // UNITS

    head = ORDER[0][0][2] * unit
    loads = (
        (
            (low_gate, v_low_gate),
            (high_gate, v_high_gate),
            (w_gate.at[:, pl.ds(0, head)], v_gate.at[:, pl.ds(0, head)]),
        ),
        ((w_gate.at[:, pl.ds(head, tall - head)], v_gate.at[:, pl.ds(head, tall - head)]),),
        ((low_up, v_low_up), (high_up, v_high_up), (w_up, v_up)),
        ((low_down, v_low_down), (high_down, v_high_down), (w_down, v_down)),
        ((train, v_train),),
        ((step, v_step),),
    )
    for i, pairs in enumerate(loads):
        for src, dst in pairs:
            pltpu.make_async_copy(src, dst, load_sem.at[i]).start()

    def bulk(elements):
        return o_gate.at[pl.ds(0, elements // o_gate.shape[1])]

    def loaded(i):
        if len(loads[i]) == 1:
            pltpu.make_async_copy(*loads[i][0], load_sem.at[i]).wait()
        else:
            ref = bulk(sum(math.prod(dst.shape) for _, dst in loads[i]))
            pltpu.make_async_copy(ref, ref, load_sem.at[i]).wait()

    def target(way):
        return {UP: me + X, DOWN: me - X, SIDE: partner}[way]

    def has(way):
        return {UP: z + 1 < lines, DOWN: z > 0, SIDE: None}[way]

    barrier = pltpu.get_barrier_semaphore()
    peers = [lax.rem(w + k, widths) for k in range(1, widths)]
    after = [w + k < widths for k in range(1, widths)]

    def signal(sem, dev):
        pl.semaphore_signal(sem, inc=1, device_id=dev, device_id_type=MESH)

    when(has(UP), lambda: signal(barrier, (target(UP), w)))
    pl.when(x == 0)(lambda: signal(barrier, (partner, w)))
    for p, later in zip(peers, after):
        pl.when(later)(lambda p=p: signal(barrier, (me, p)))

    def enter():
        before = jnp.where(z > 0, 1, 0) + x + w
        pl.when(before > 0)(lambda: pl.semaphore_wait(barrier, before))
        when(has(DOWN), lambda: signal(ready.at[UP], (target(DOWN), w)))
        pl.when(x == 1)(lambda: signal(ready.at[SIDE], (partner, w)))
        for p, later in zip(peers, after):
            pl.when(jnp.logical_not(later))(lambda p=p: signal(ready.at[WIDE], (me, p)))

    def place(s, c):
        t, first, n = c
        block = pl.ds(pl.multiple_of(s * wide, wide), wide)
        inner = pl.ds(first * unit, n * unit)
        return outs[t].at[inner, block] if t < 2 else outs[t].at[block, inner]

    def share(t):
        return 0 if t in SHARES[0] else 1

    def receipt(way, plane, whole, extra):
        if extra:
            return extra_sem.at[0 if way == SIDE else 1]
        if way == SIDE:
            return extra_sem.at[2 + PAIR.index(whole)] if whole in PAIR else side_sem.at[share(whole[0])]
        slot = plane if way == UP else plane - 1
        for i, bundle in enumerate(BUNDLES):
            if whole in bundle:
                return line_sem.at[slot * len(BUNDLES) + i]
        return pair_sem.at[slot * 2 + (1 if whole == LATE_PAIR else 0)]

    def remote(way, s, c, whole, extra=False):
        return pltpu.make_async_remote_copy(
            src_ref=place(s, c),
            dst_ref=place(s, c),
            send_sem=send_sem.at[way * len(SHARES) + share(c[0])],
            recv_sem=receipt(way, s // X, whole, extra),
            device_id=(target(way), w),
            device_id_type=MESH,
        )

    def send(way, s, c, cond=None, whole=None, extra=False):
        when(both(cond, has(way)), lambda: remote(way, s, c, whole or c, extra).start())

    def bytes_of(units, send, recv):
        ref = bulk(units * unit * wide)
        return pltpu.make_async_remote_copy(
            src_ref=ref, dst_ref=ref, send_sem=send, recv_sem=recv, device_id=(partner, w), device_id_type=MESH
        )

    def arrive(way, plane, pieces, cond=None, extra=False):
        sem = receipt(way, plane, pieces[0], extra)
        when(cond, lambda: bytes_of(units_of(pieces), send_sem.at[0], sem).wait_recv())

    def drain(way, i, units):
        bytes_of(units, send_sem.at[way * len(SHARES) + i], side_sem.at[i]).wait_send()

    def collect(i, units):
        bytes_of(units, send_sem.at[i], side_sem.at[i]).wait_recv()

    seen = set()

    def compute(c):
        t, first, n = c
        if t not in seen:
            seen.add(t)
            loaded((0, 2, 3)[t])
            if t == 0:
                l_gate[...] = v_low_gate[...].T
            elif t == 1:
                l_up[...] = v_low_up[...].T
            else:
                h_down[...] = v_high_down[...].T
        elif c == ORDER[1][0]:
            loaded(1)
        columns = pl.ds(pl.multiple_of(me * wide, wide), wide)

        @pl.loop(0, n * unit // LANES)
        def _(i):
            at = pl.ds(pl.multiple_of(first * unit + i * LANES, LANES), LANES)
            if t < 2:
                block, low, high = ((v_gate, l_gate, v_high_gate), (v_up, l_up, v_high_up))[t]
                outs[t][at, columns] = merged(block[:, at], low[...], high[:, at]).T
            else:
                o_down[columns, at] = merged(v_down[at, :].T, h_down[...], v_low_down[:, at])

    for k, (c, whole) in enumerate(ORDER):
        compute(c)
        if k == 0:
            enter()
        if whole in LINE:
            send(DOWN, me, c, None, whole)
        if k == 0:
            pl.when(x == 0)(lambda: pl.semaphore_wait(ready.at[SIDE], 1))
        send(SIDE, me, c, None, whole, c == LATE_LINE)
        if k == 0:
            when(has(UP), lambda: pl.semaphore_wait(ready.at[UP], 1))
        if whole in LINE:
            send(UP, me, c, None, whole)

    def norm_rows(begin, count):
        return o_norm.at[pl.ds(begin, count)]

    def norm_copy(begin, count, sem, rsem, dev):
        return pltpu.make_async_remote_copy(
            src_ref=norm_rows(begin, count), dst_ref=norm_rows(begin, count),
            send_sem=norm_send.at[sem], recv_sem=norm_recv.at[rsem],
            device_id=dev, device_id_type=MESH,
        )

    loaded(4)
    loaded(5)
    gain = v_train[...] + v_step[...]
    row = jnp.concatenate([gain] * (LANES // gain.shape[1]), axis=1)
    o_norm[pl.ds(me * widths + w, 1)] = row.reshape(1, 1, LANES)
    pl.when(w + 1 < widths)(lambda: pl.semaphore_wait(ready.at[WIDE], widths - 1 - w))
    for p in peers:
        norm_copy(me * widths + w, 1, 3, 0, (me, p)).start()
    tiles = lambda: norm_copy(0, widths - 1, 3, 0, (partner, w))
    norm_side = lambda s: norm_copy(s * widths, widths, SIDE, 1, (partner, w))
    plane_rows = X * widths
    norm_plane = lambda way, plane: norm_copy(
        plane * plane_rows, plane_rows, way, 2 + (plane if way == UP else plane - 1), (target(way), w)
    )
    if widths > 1:
        tiles().wait_recv()
    norm_side(me).start()

    far = far_plane(z, lines)
    inner = jnp.logical_and(z > 0, z + 1 < lines)
    lower = z < lines // 2
    mate = jnp.where(lower, z + 1, z - 1)
    lends = {
        DOWN: jnp.logical_and(z >= 2, z - 1 < lines // 2),
        UP: jnp.logical_and(z + 1 >= lines // 2, z + 2 < lines),
    }

    def by_side(plane):
        return jnp.logical_and(plane != far, jnp.logical_not(jnp.logical_and(inner, plane == mate)))

    def lend():
        arrive(SIDE, z, (LATE_LINE,), None, True)
        for way in (UP, DOWN):
            send(way, partner, LATE_LINE, lends[way], None, True)

    def hops(d):
        return ((UP, z - d, z >= d), (DOWN, z + d, z + d < lines))

    def forward_line(d):
        for pieces in BUNDLES:
            for way, plane, cond in hops(d):
                arrive(way, plane, pieces, cond)
                for c in pieces:
                    send(way, plane * X + x, c, cond)
                    send(SIDE, plane * X + x, c, both(cond, by_side(plane)) if c == LATE_LINE else cond)

    source = {UP: 0, DOWN: lines - 1}
    feeds = {UP: z == lines - 2, DOWN: z == 1}

    def send_pair(way, plane, j, c, cond=None):
        if c == LATE_PAIR:
            late = jnp.logical_and(feeds[way], plane == source[way])
            cond = both(cond, jnp.logical_not(late))
        send(way, plane * X + (x + j) % X, c, cond)

    def arrive_pair(way, plane, pieces, cond):
        if LATE_PAIR in pieces:
            end = {UP: z == lines - 1, DOWN: z == 0}[way]
            late = jnp.logical_and(end, plane == source[way])
            cond = both(cond, jnp.logical_not(late))
        arrive(way, plane, pieces, cond)

    def forward_pair(d):
        if d == 0:
            send(UP, me, WHOLE)
            send(DOWN, me, WHOLE)
            norm_side(partner).wait_recv()
            for way in (UP, DOWN):
                when(has(way), lambda way=way: norm_plane(way, z).start())
            for c in PAIR:
                arrive(SIDE, z, (c,))
                send_pair(UP, z, 1, c)
                send_pair(DOWN, z, 1, c)
            return
        for way, plane, cond in hops(d):
            when(cond, lambda way=way, plane=plane: norm_plane(way, plane).wait_recv())
            when(both(cond, has(way)), lambda way=way, plane=plane: norm_plane(way, plane).start())
        for bundle in (((WHOLE, 0), (PAIR[0], 1)), ((LATE_PAIR, 1),)):
            for way, plane, cond in hops(d):
                arrive_pair(way, plane, [c for c, _ in bundle], cond)
                for c, j in bundle:
                    send_pair(way, plane, j, c, cond)

    for d in range(1, lines):
        forward_line(d)
        forward_pair(d - 1)
        if d == 1:
            lend()
    bridge = jnp.logical_or(z == 1, z == lines - 2)
    keep = jnp.where(z == 1, lines - 1, 0) * X + (1 - x)
    keep = jnp.where(bridge, keep, me)
    late_x[...] = place(far * X + x, LATE_LINE)[...]
    late_z[...] = place(keep, LATE_PAIR)[...]
    forward_pair(lines - 1)

    arrive(DOWN, mate, (LATE_LINE,), inner, True)
    lent = share(LATE_LINE[0])
    for i, arrays in enumerate(SHARES):
        units = lines * units_of(LINE, arrays)
        own = units_of(PAIR, arrays)
        if i != lent:
            collect(i, units)
            drain(SIDE, i, units + own)
            continue
        for cond, skipped in ((inner, 2 * LATE_LINE[2]), (jnp.logical_not(inner), LATE_LINE[2])):

            @pl.when(cond)
            def _(i=i, units=units - skipped, own=own):
                collect(i, units - LATE_LINE[2])
                drain(SIDE, i, units + own)
    norm_side(me).wait_send()
    if widths > 1:
        tiles().wait_send()
    for way in (UP, DOWN):
        for k in range(lines):
            planes = k + 1 if way == UP else lines - k
            if planes == lines:
                continue

            @pl.when(both(z == k, has(way)))
            def _(way=way, planes=planes):
                feeder = k == (lines - 2 if way == UP else 1)
                lends_here = (k >= 2 and k - 1 < lines // 2) if way == DOWN else (k + 1 >= lines // 2 and k + 2 < lines)
                for i, arrays in enumerate(SHARES):
                    units = planes * (units_of(LINE, arrays) + X * units_of(PAIR, arrays))
                    units -= LATE_PAIR[2] * (feeder and i == share(LATE_PAIR[0]))
                    units += LATE_LINE[2] * (lends_here and i == lent)
                    drain(way, i, units)
                norm_copy(0, planes * plane_rows, way, 0, (partner, w)).wait_send()


def gather_all(shards, widths, args):
    lines = shards // X
    w_gate, low_gate, high_gate, w_up, low_up, high_up, w_down, low_down, high_down, train, step = args
    hbm = pl.BlockSpec(memory_space=pltpu.HBM)
    vmem = pl.BlockSpec(memory_space=pltpu.VMEM)
    like = lambda a: pltpu.VMEM(a.shape, a.dtype)
    flip = lambda a: pltpu.VMEM(a.shape[::-1], a.dtype)
    wide, tall = w_gate.shape
    full = pltpu.VMEM((tall, shards * wide), w_gate.dtype)
    return pl.pallas_call(
        functools.partial(gather_kernel, shards, widths),
        out_shape=(
            full, full,
            pltpu.VMEM((shards * wide, tall), w_down.dtype),
            pltpu.VMEM((shards * widths, 1, LANES), train.dtype),
            pltpu.VMEM((wide, LATE_LINE[2] * tall // UNITS), w_down.dtype),
            pltpu.VMEM((LATE_PAIR[2] * tall // UNITS, wide), w_up.dtype),
        ),
        in_specs=[hbm] * len(args),
        out_specs=(vmem,) * 6,
        scratch_shapes=[
            like(w_gate), like(w_up), like(w_down),
            like(low_gate), like(low_up), like(low_down),
            like(high_gate), like(high_up), like(high_down),
            like(train), like(step),
            flip(low_gate), flip(low_up), flip(high_down),
            pltpu.SemaphoreType.DMA((WAYS * len(SHARES),)),
            pltpu.SemaphoreType.DMA(((lines - 1) * len(BUNDLES),)),
            pltpu.SemaphoreType.DMA(((lines - 1) * 2,)),
            pltpu.SemaphoreType.DMA((len(SHARES),)),
            pltpu.SemaphoreType.DMA((2 + len(PAIR),)),
            pltpu.SemaphoreType.DMA((4,)),
            pltpu.SemaphoreType.DMA((1 + lines,)),
            pltpu.SemaphoreType.DMA((6,)),
            pltpu.SemaphoreType.REGULAR((3,)),
        ],
        compiler_params=pltpu.CompilerParams(collective_id=0, has_side_effects=True, vmem_limit_bytes=16 * 2**20),
    )(*(pltpu.with_memory_space_constraint(a, pltpu.HBM) for a in args))


def write_kernel(gate, up, down, rows, o_gate, o_up, o_down, o_norm, norm, sem):
    pairs = ((gate, o_gate), (up, o_up), (down, o_down))
    part = gate.shape[0] // WRITES
    copies = [
        pltpu.make_async_copy(a.at[pl.ds(j * part, part)], b.at[pl.ds(j * part, part)], sem.at[i])
        for i, (a, b) in enumerate(pairs)
        for j in range(WRITES)
    ]
    for copy in copies:
        copy.start()
    per = rows.shape[1]
    lane = lax.broadcasted_iota(jnp.int32, norm.shape, 1) // (LANES // per)
    line = rows[:, 0, :]
    for j in range(1, per):
        line = jnp.where(lane == j, rows[:, j, :], line)
    norm[...] = line.astype(norm.dtype)
    last = pltpu.make_async_copy(norm, o_norm, sem.at[len(pairs)])
    last.start()
    for i, (a, b) in enumerate(pairs):
        pltpu.make_async_copy(a, b, sem.at[i]).wait()
    last.wait()


def write_out(gate, up, down, rows):
    any_ = pl.BlockSpec(memory_space=pl.ANY)
    vmem = pl.BlockSpec(memory_space=pltpu.VMEM)
    norm = (rows.shape[0], LANES)
    return pl.pallas_call(
        write_kernel,
        out_shape=tuple(jax.ShapeDtypeStruct(a.shape, a.dtype) for a in (gate, up, down))
        + (jax.ShapeDtypeStruct(norm, jnp.bfloat16),),
        in_specs=[any_] * 3 + [vmem],
        out_specs=(any_,) * 4,
        scratch_shapes=[pltpu.VMEM(norm, jnp.bfloat16), pltpu.SemaphoreType.DMA((4,))],
        cost_estimate=pl.CostEstimate(flops=WRITE_FLOPS, bytes_accessed=2 * 3 * gate.size * 2, transcendentals=0),
        compiler_params=pltpu.CompilerParams(vmem_limit_bytes=4 * 2**20),
    )(gate, up, down, rows)


def late_kernel(lines, up, down, late_z, late_x, o_up, o_down, sem):
    me = lax.axis_index("shard")
    z, x = me // X, me % X
    wide, tall = late_z.shape[1], up.shape[0]
    unit = tall // UNITS
    end = jnp.logical_or(z == 0, z == lines - 1)
    block = (far_plane(z, lines) * X + (1 - x)) * wide
    block = pl.ds(pl.multiple_of(block, wide), wide)
    inner = lambda c: pl.ds(c[1] * unit, c[2] * unit)
    put_x = pltpu.make_async_copy(late_x, o_down.at[block, inner(LATE_LINE)], sem.at[0])
    put_z = pltpu.make_async_copy(late_z, o_up.at[inner(LATE_PAIR), block], sem.at[1])
    put_x.start()
    pl.when(end)(put_z.start)
    put_x.wait()
    pl.when(end)(put_z.wait)


def write_late(lines, up, down, late_x, late_z):
    any_ = pl.BlockSpec(memory_space=pl.ANY)
    vmem = pl.BlockSpec(memory_space=pltpu.VMEM)
    return pl.pallas_call(
        functools.partial(late_kernel, lines),
        out_shape=tuple(jax.ShapeDtypeStruct(a.shape, a.dtype) for a in (up, down)),
        in_specs=[any_] * 2 + [vmem] * 2,
        out_specs=(any_,) * 2,
        input_output_aliases={0: 0, 1: 1},
        scratch_shapes=[pltpu.SemaphoreType.DMA((2,))],
        compiler_params=pltpu.CompilerParams(vmem_limit_bytes=4 * 2**20),
    )(up, down, late_z, late_x)


def body(
    shards,
    widths,
    w_gate,
    low_gate,
    high_gate,
    w_up,
    low_up,
    high_up,
    w_down,
    low_down,
    high_down,
    norm_train,
    norm_step,
):
    count = norm_train.shape[0]
    wide, tall = w_gate.shape
    if shards % (2 * X) or shards > 4 * X or wide % LANES or tall % (UNITS * LANES) or LANES % count or (shards * widths * count) % LANES:
        gate = merged(w_gate, low_gate, high_gate)
        up = merged(w_up, low_up, high_up)
        down = merged(w_down, low_down, high_down)
        gate, up, down = (
            lax.all_gather(gate, "shard", axis=0, tiled=True),
            lax.all_gather(up, "shard", axis=0, tiled=True),
            lax.all_gather(down, "shard", axis=1, tiled=True),
        )
        gain = (norm_train + norm_step).astype(jnp.bfloat16)
        gain = lax.all_gather(gain, ("shard", "width"), axis=0, tiled=True)
        return gate.T, up.T, down.T, gain
    args = (
        w_gate, low_gate.T, high_gate, w_up, low_up.T, high_up, w_down, low_down.T, high_down,
        norm_train.reshape(1, count), norm_step.reshape(1, count),
    )
    gate, up, down, rows, late_x, late_z = gather_all(shards, widths, args)
    per = LANES // count
    late_z = lax.ppermute(late_z, "shard", [(s, s ^ X) for s in range(shards)])
    late_x = lax.ppermute(late_x, "shard", [(s, s ^ 1) for s in range(shards)])
    gate, up, down, norm = write_out(gate, up, down, rows.reshape(-1, per, LANES))
    up, down = write_late(shards // X, up, down, late_x, late_z)
    return gate, up, down, norm.reshape(-1)


def solution(mesh):
    return jax.shard_map(
        functools.partial(body, mesh.shape["shard"], mesh.shape["width"]),
        mesh=mesh,
        in_specs=(
            P("shard", "width"),
            P("shard", None),
            P(None, "width"),
            P("shard", "width"),
            P("shard", None),
            P(None, "width"),
            P("width", "shard"),
            P("width", None),
            P(None, "shard"),
            P(("shard", "width")),
            P(("shard", "width")),
        ),
        out_specs=(P("width", None), P("width", None), P(None, "width"), P()),
        check_vma=False,
    )
```
